32 devices in a mesh: row: 4 (over y, x), col: 8 (over z, core).
Axes of the slice: x: 2, y: 2, z: 4, core: 2. Of those that a mesh axis runs over, the one named last changes fastest.
Arguments:
- b_diag: float32 [512, 512], P('row'), as said below
- a_diag: float32 [512, 512], P('row'), as said below
- b_panel: float32 [1024, 512], P(('row', 'col')), may hold values from -2 to 2
- a_panel: float32 [1024, 512], P(('row', 'col')), may hold values from -2 to 2
- a_trail: float32 [1024, 1024], P('row', 'col'), as said below
Outputs:
- a_diag_new: float32 [512, 512], P('row')
- l_panel: float32 [1024, 512], P(('row', 'col'))
- a_panel_new: float32 [1024, 512], P(('row', 'col'))
- a_trail_new: float32 [1024, 1024], P('row', 'col')
The draws below stay inside these ranges and needn't reach their ends.
Inputs may be any that keep to these rules, and one draw needn't show every extreme that they name: b_diag is symmetric positive definite, its smallest eigenvalue 0.5 or more. a_diag is symmetric. a_trail is symmetric.
All inputs are finite; a program needn't handle non-finite values.
Results may differ from the reference program's by a relative error of at most 0.0001.
Values sent between devices are 32-bit elements; how exact they have to be, the bound alone decides.
No kernel may reach another device: no remote copies, remote signals or barrier semaphores. Data moves between devices by JAX's collectives and lax.ppermute only.
A program may use at most 64 MiB of HBM per device.

```python
import jax
import jax.numpy as jnp
from jax import lax

NB = 512
ORDER = 1024


def draw_b_diag(key, part):
    first = jax.random.fold_in(key, 11)
    second = jax.random.fold_in(key, 12)
    factor_rows = jax.random.normal(first, (NB, NB), jnp.float32) * (0.7 / NB ** 0.5)
    shifts = jax.random.uniform(second, (NB,), jnp.float32, 0.5, 1.5)
    product = jnp.dot(factor_rows, factor_rows.T, precision=lax.Precision.HIGHEST)
    return 0.5 * (product + product.T) + jnp.diag(shifts)


def draw_a_diag(key, part):
    values = jax.random.normal(jax.random.fold_in(key, 21), (NB, NB), jnp.float32)
    return (values + values.T) * (0.05 / 2.0 ** 0.5)


def draw_a_trail(key, part):
    values = jax.random.normal(jax.random.fold_in(key, 31), (ORDER, ORDER), jnp.float32)
    return (values + values.T) * (0.5 / 2.0 ** 0.5)


def level_of(key, dims, cuts, low, high):
    level = 1.0
    for axis_at, parts in cuts:
        heights = jax.random.uniform(jax.random.fold_in(jax.random.fold_in(key, 6), axis_at), (parts,), jnp.float32, low / len(cuts), high / len(cuts))
        level = level * jnp.repeat(jnp.exp(heights), dims[axis_at] // parts).reshape((-1,) + (1,) * (len(dims) - 1 - axis_at))
    return level


def scatter_about(own_key, shape, deviation, limit, cuts=(), kind=jnp.bfloat16):
    result = jax.random.normal(own_key, shape, jnp.float32) * deviation
    if len(cuts) > 0:
        result = level_of(own_key, shape, cuts, -0.22, 0.18) * result
    return jnp.clip(result, min=-limit, max=limit).astype(kind)


def setup_inputs(seed: int = 0) -> dict:
    streams_of = jax.random.split(jax.random.key(seed), 6)
    b_diag = draw_b_diag(jax.random.fold_in(streams_of[5], 71), 0)
    a_diag = draw_a_diag(jax.random.fold_in(streams_of[5], 71), 0)
    b_panel = scatter_about(streams_of[2], (ORDER, NB), 0.3, 2.0, ((0, 32),), jnp.float32)
    a_panel = scatter_about(streams_of[3], (ORDER, NB), 0.3, 2.0, ((0, 32),), jnp.float32)
    a_trail = draw_a_trail(jax.random.fold_in(streams_of[5], 71), 0)
    return dict(b_diag=b_diag, a_diag=a_diag, b_panel=b_panel, a_panel=a_panel, a_trail=a_trail)


HIGHEST = lax.Precision.HIGHEST

def matmul(left, right):
    return jnp.dot(left.astype(jnp.float32), right.astype(jnp.float32), precision=HIGHEST, preferred_element_type=jnp.float32)

def reference(b_diag, a_diag, b_panel, a_panel, a_trail):
    factor = jnp.linalg.cholesky(b_diag)
    identity = jnp.eye(b_diag.shape[0], dtype=b_diag.dtype)
    inverse = jax.scipy.linalg.solve_triangular(factor, identity, lower=True)
    a_diag_new = matmul(matmul(inverse, a_diag), inverse.T)
    l_panel = matmul(b_panel, inverse.T)
    correction = 0.5 * matmul(l_panel, a_diag_new)
    mixed = matmul(a_panel, inverse.T) - correction
    a_trail_new = a_trail - matmul(mixed, l_panel.T) - matmul(l_panel, mixed.T)
    a_panel_new = mixed - correction
    return (a_diag_new, l_panel, a_panel_new, a_trail_new)
```

```python
import functools

import jax
import jax.numpy as jnp
from jax import lax
from jax.experimental import pallas as pl
from jax.experimental.pallas import tpu as pltpu
from jax.sharding import Mesh
from jax.sharding import PartitionSpec as P


HIGHEST = lax.Precision.HIGHEST
SMALL = 32
BLOCK = 128
VMEM = pl.BlockSpec(memory_space=pltpu.VMEM)
SMEM = pl.BlockSpec(memory_space=pltpu.SMEM)


def nt(left, right):
    return lax.dot_general(
        left, right, (((1,), (1,)), ((), ())), precision=HIGHEST, preferred_element_type=jnp.float32
    )


def nn(left, right):
    return lax.dot_general(
        left, right, (((1,), (0,)), ((), ())), precision=HIGHEST, preferred_element_type=jnp.float32
    )


def invert_small(block, offset):
    lanes = block.shape[1]
    groups = SMALL // 8
    cols = []
    for m in range(SMALL):
        column = block[:, offset + m : offset + m + 1]
        cols.append(
            [
                jnp.broadcast_to(column[8 * h : 8 * h + 8], (8, lanes)) if h >= m // 8 else None
                for h in range(groups)
            ]
        )
    sublane = lax.broadcasted_iota(jnp.int32, (8, lanes), 0)
    lane = lax.broadcasted_iota(jnp.int32, (8, lanes), 1)
    rows = [jnp.where(lane == sublane + (offset + 8 * h), 1.0, 0.0).astype(jnp.float32) for h in range(groups)]
    pivots = [None] * groups

    def spread_row(value, s):
        return jnp.broadcast_to(value[s : s + 1, :], (8, lanes))

    for j in range(SMALL):
        g = j // 8
        c = cols[j]
        pivot = spread_row(c[g], j % 8)
        scale = 1.0 / pivot
        pivots[g] = pivot if j % 8 == 0 else jnp.where(sublane == j % 8, pivot, pivots[g])
        row = spread_row(rows[g], j % 8)
        low = [None if c[h] is None else c[h] * scale for h in range(groups)]
        for m in range(j + 1, SMALL):
            t = spread_row(c[m // 8], m % 8)
            for h in range(m // 8, groups):
                if m == j + 1:
                    cols[m][h] = cols[m][h] - (c[h] * t) * scale
                else:
                    cols[m][h] = cols[m][h] - low[h] * t
        for h in range(g, groups):
            factor = jnp.where(sublane > j % 8, low[h], 0.0) if h == g else low[h]
            rows[h] = rows[h] - factor * row
    return jnp.concatenate([rows[h] * lax.rsqrt(pivots[h]) for h in range(groups)], axis=0)


def invert_block(block):
    size = block.shape[0]
    done = []
    total = None
    for b in range(size // SMALL):
        offset = b * SMALL
        below = offset + SMALL
        small = invert_small(block[offset:below, :], offset)
        last = below == size
        if not last:
            low = nt(block[below:, :], small)
            full = jnp.concatenate([jnp.zeros((below, SMALL), jnp.float32), low], axis=0)
            block = jnp.concatenate([block[:below], block[below:, :] - nt(low, full)], axis=0)
        strip = small if total is None else small - nn(small, total)
        done.append(strip)
        if not last:
            update = nn(full, strip)
            total = update if total is None else total + update
    return jnp.concatenate(done, axis=0)


def factor_kernel(shifts, row_ref, *refs):
    pieces, (out_ref, work, sums) = refs[:shifts], refs[shifts:]
    size = out_ref.shape[0]
    height = pieces[0].shape[0]
    me = row_ref[0]
    for s in range(shifts):
        source = lax.rem(me - s + shifts, shifts)
        work[pl.ds(pl.multiple_of(source * height, 8), height), :] = pieces[s][...]
    count = size // BLOCK
    out_ref[...] = jnp.zeros_like(out_ref)
    for k in range(count):
        lo, hi = k * BLOCK, (k + 1) * BLOCK
        inverse = invert_block(work[lo:hi, lo:hi])
        out_ref[lo:hi, lo:hi] = inverse
        if hi < size:
            low = nt(work[hi:, lo:hi], inverse)
            for i in range(k + 1, count):
                part = slice(i * BLOCK, (i + 1) * BLOCK)
                mine = low[i * BLOCK - hi : (i + 1) * BLOCK - hi]
                work[part, hi : (i + 1) * BLOCK] = work[part, hi : (i + 1) * BLOCK] - nt(mine, low[: (i + 1) * BLOCK - hi])
        if k > 0:
            out_ref[lo:hi, :lo] = -nn(inverse, sums[lo:hi, :lo])
        if hi < size:
            update = nn(low, out_ref[lo:hi, :hi])
            if k > 0:
                sums[hi:, :lo] = sums[hi:, :lo] + update[:, :lo]
            sums[hi:, lo:hi] = update[:, lo:hi]


def invert_factor(row, pieces):
    size = pieces[0].shape[1]
    return pl.pallas_call(
        functools.partial(factor_kernel, len(pieces)),
        out_shape=jax.ShapeDtypeStruct((size, size), jnp.float32),
        in_specs=[SMEM] + [VMEM] * len(pieces),
        out_specs=VMEM,
        scratch_shapes=[pltpu.VMEM((size, size), jnp.float32)] * 2,
        cost_estimate=pl.CostEstimate(flops=100 * size**3, bytes_accessed=8 * size * size, transcendentals=0),
    )(row, *pieces)


def split(value):
    high = value.astype(jnp.bfloat16)
    return high, (value - high.astype(jnp.float32)).astype(jnp.bfloat16)


def product(left, right, dims):
    def dot(x, y):
        return lax.dot_general(x, y, (dims, ((), ())), preferred_element_type=jnp.float32)

    return dot(left[0], right[0]) + (dot(left[0], right[1]) + dot(left[1], right[0]))


NT = ((1,), (1,))
NN = ((1,), (0,))


def update_kernel(shifts, place_ref, *refs):
    inverse_ref, own_ref, other_ref, trail_ref = refs[:4]
    diag = refs[4 : 4 + shifts]
    received = refs[4 + shifts : 4 + 2 * shifts]
    diag_out, low_out, panel_out, trail_out, diag_work, rows_work, cols_work = refs[4 + 2 * shifts :]
    row, core, hop, place, start = (place_ref[i] for i in range(5))
    chips, _, rows, size = own_ref.shape
    height = diag[0].shape[0]
    for s in range(shifts):
        source = lax.rem(row - s + shifts, shifts)
        diag_work[pl.ds(pl.multiple_of(source * height, 8), height), :] = diag[s][...]
    for z in range(chips):
        for which in range(2):
            rows_work[which, pl.ds(pl.multiple_of((z * 2 + core) * rows, 8), rows), :] = own_ref[z, which]
            rows_work[which, pl.ds(pl.multiple_of((z * 2 + 1 - core) * rows, 8), rows), :] = other_ref[z, which]
    for s in range(shifts):

        @pl.when(hop == s)
        def _():
            pairs = received[s].shape[1]
            for z in range(pairs):
                for which in range(2):
                    cols_work[which, pl.ds(pl.multiple_of((z * 2 + core) * rows, 8), rows), :] = received[s][0, z, which]
                    cols_work[which, pl.ds(pl.multiple_of((z * 2 + 1 - core) * rows, 8), rows), :] = received[s][1, z, which]

    inverse = split(inverse_ref[...])
    half = split(product(inverse, split(diag_work[...]), NN))
    reduced = product(half, inverse, NT)
    diag_work[...] = reduced
    diag_out[...] = diag_work[pl.ds(pl.multiple_of(row * height, 8), height), :]
    reduced = split(reduced)

    def panel(work):
        low = product(split(work[0]), inverse, NT)
        correction = 0.5 * product(split(low), reduced, NN)
        mixed = product(split(work[1]), inverse, NT) - correction
        return low, mixed, correction

    low_rows, mixed_rows, correction = panel(rows_work)
    rows_work[0] = low_rows
    rows_work[1] = mixed_rows - correction
    mine = pl.ds(pl.multiple_of(place * rows, 8), rows)
    low_out[...] = rows_work[0, mine, :]
    panel_out[...] = rows_work[1, mine, :]
    low_cols, mixed_cols, _ = panel(cols_work)
    trail_out[...] = trail_ref[...] - (
        product(split(mixed_rows), split(low_cols), NT) + product(split(low_rows), split(mixed_cols), NT)
    )


def shards(b_diag, a_diag, b_panel, a_panel, a_trail):
    count, chips, cores = (lax.axis_size(name) for name in ("row", "chip", "core"))
    row, chip, core = (lax.axis_index(name) for name in ("row", "chip", "core"))
    rows, size = b_panel.shape
    height, width = a_trail.shape

    def rotations(array):
        return [array] + [
            lax.ppermute(array, "row", [(i, (i + s) % count) for i in range(count)]) for s in range(1, count)
        ]

    b_pieces = rotations(b_diag)
    stacked = jnp.stack([b_panel, a_panel])
    own = lax.all_gather(stacked, "chip", axis=0)
    other = lax.ppermute(own, "core", [(0, 1), (1, 0)])
    a_pieces = rotations(a_diag)
    col = chip * cores + core
    source_row = col * width // height
    start = col * width - source_row * height
    pairs = width // (cores * rows)
    first = jnp.clip(start // (cores * rows), 0, chips - pairs)
    outgoing = jnp.stack([lax.dynamic_slice_in_dim(x, first, pairs, 0) for x in (own, other)])

    def sources(s):
        found = []
        for c in range(chips * cores):
            origin = c * width // height
            target = (origin + s) % count
            found.append((origin * chips * cores + c, target * chips * cores + c))
        return found

    col_pieces = [outgoing] + [
        lax.ppermute(outgoing, ("row", "chip", "core"), sources(s)) for s in range(1, count)
    ]
    inverse = invert_factor(row[None], b_pieces)
    hop = lax.rem(row - source_row + count, count)
    places = jnp.stack([row, core, hop, col, first]).astype(jnp.int32)
    shape = jax.ShapeDtypeStruct
    return pl.pallas_call(
        functools.partial(update_kernel, count),
        out_shape=(
            shape(a_diag.shape, jnp.float32),
            shape((rows, size), jnp.float32),
            shape((rows, size), jnp.float32),
            shape(a_trail.shape, jnp.float32),
        ),
        in_specs=[SMEM] + [VMEM] * (4 + 2 * count),
        out_specs=(VMEM,) * 4,
        scratch_shapes=[
            pltpu.VMEM((size, size), jnp.float32),
            pltpu.VMEM((2, height, size), jnp.float32),
            pltpu.VMEM((2, width, size), jnp.float32),
        ],
        cost_estimate=pl.CostEstimate(flops=10 * size**3, bytes_accessed=8 * size * size, transcendentals=0),
    )(places, inverse, own, other, a_trail, *a_pieces, *col_pieces)


def solution(mesh):
    count, cols = mesh.devices.shape
    cores = 2
    fine = Mesh(mesh.devices.reshape(count, cols // cores, cores), ("row", "chip", "core"))
    in_specs = (
        P("row", None),
        P("row", None),
        P(("row", "chip", "core"), None),
        P(("row", "chip", "core"), None),
        P("row", ("chip", "core")),
    )
    out_specs = (
        P("row", None),
        P(("row", "chip", "core"), None),
        P(("row", "chip", "core"), None),
        P("row", ("chip", "core")),
    )
    return jax.shard_map(shards, mesh=fine, in_specs=in_specs, out_specs=out_specs, check_vma=False)
```

```python
import functools

import jax
import jax.numpy as jnp
from jax import lax
from jax.experimental import pallas as pl
from jax.experimental.pallas import tpu as pltpu
from jax.sharding import Mesh
from jax.sharding import PartitionSpec as P


HIGHEST = lax.Precision.HIGHEST
SMALL = 32
BLOCK = 128
TOKEN = jax.ShapeDtypeStruct((8, 128), jnp.float32)
VMEM = pl.BlockSpec(memory_space=pltpu.VMEM)
SMEM = pl.BlockSpec(memory_space=pltpu.SMEM)


def memory(*elements):
    return pltpu.CompilerParams(vmem_limit_bytes=min(2**23 + 12 * sum(elements), 60 * 2**20))


def nt(left, right):
    return lax.dot_general(
        left, right, (((1,), (1,)), ((), ())), precision=HIGHEST, preferred_element_type=jnp.float32
    )


def nn(left, right):
    return lax.dot_general(
        left, right, (((1,), (0,)), ((), ())), precision=HIGHEST, preferred_element_type=jnp.float32
    )


def invert_small(block, offset):
    lanes = block.shape[1]
    groups = SMALL // 8
    cols = []
    for m in range(SMALL):
        column = block[:, offset + m : offset + m + 1]
        cols.append(
            [
                jnp.broadcast_to(column[8 * h : 8 * h + 8], (8, lanes)) if h >= m // 8 else None
                for h in range(groups)
            ]
        )
    sublane = lax.broadcasted_iota(jnp.int32, (8, lanes), 0)
    lane = lax.broadcasted_iota(jnp.int32, (8, lanes), 1)
    rows = [jnp.where(lane == sublane + (offset + 8 * h), 1.0, 0.0).astype(jnp.float32) for h in range(groups)]
    pivots = [None] * groups

    def spread_row(value, s):
        return jnp.broadcast_to(value[s : s + 1, :], (8, lanes))

    for j in range(SMALL):
        g = j // 8
        c = cols[j]
        pivot = spread_row(c[g], j % 8)
        scale = 1.0 / pivot
        pivots[g] = pivot if j % 8 == 0 else jnp.where(sublane == j % 8, pivot, pivots[g])
        row = spread_row(rows[g], j % 8)
        low = [None if c[h] is None else c[h] * scale for h in range(groups)]
        for m in range(j + 1, SMALL):
            t = spread_row(c[m // 8], m % 8)
            for h in range(m // 8, groups):
                if m == j + 1:
                    cols[m][h] = cols[m][h] - (c[h] * t) * scale
                else:
                    cols[m][h] = cols[m][h] - low[h] * t
        for h in range(g, groups):
            factor = jnp.where(sublane > j % 8, low[h], 0.0) if h == g else low[h]
            rows[h] = rows[h] - factor * row
    return jnp.concatenate([rows[h] * lax.rsqrt(pivots[h]) for h in range(groups)], axis=0)


def invert_block(block):
    size = block.shape[0]
    done = []
    total = None
    for b in range(size // SMALL):
        offset = b * SMALL
        below = offset + SMALL
        small = invert_small(block[offset:below, :], offset)
        last = below == size
        if not last:
            low = nt(block[below:, :], small)
            full = jnp.concatenate([jnp.zeros((below, SMALL), jnp.float32), low], axis=0)
            block = jnp.concatenate([block[:below], block[below:, :] - nt(low, full)], axis=0)
        strip = small if total is None else small - nn(small, total)
        done.append(strip)
        if not last:
            update = nn(full, strip)
            total = update if total is None else total + update
    return jnp.concatenate(done, axis=0)


def factor_steps(work, sums, out_ref, base, first, last, count):
    start = first * BLOCK
    for k in range(first, last):
        lo, hi = k * BLOCK, (k + 1) * BLOCK
        here = slice(lo - base, hi - base)
        rows = slice(lo - start, hi - start)
        inverse = invert_block(work[here, here])
        out_ref[rows, lo:hi] = inverse
        if k + 1 < count:
            below = slice(hi - base, count * BLOCK - base)
            low = nt(work[below, here], inverse)
            for i in range(k + 1, count):
                part = slice(i * BLOCK - base, (i + 1) * BLOCK - base)
                wide = slice(hi - base, (i + 1) * BLOCK - base)
                mine = low[i * BLOCK - hi : (i + 1) * BLOCK - hi]
                work[part, wide] = work[part, wide] - nt(mine, low[: (i + 1) * BLOCK - hi])
        if k > 0:
            out_ref[rows, :lo] = -nn(inverse, sums[here, :lo])
        if k + 1 < count:
            update = nn(low, out_ref[rows, :hi])
            if k > 0:
                sums[below, :lo] = sums[below, :lo] + update[:, :lo]
            sums[below, lo:hi] = update[:, lo:hi]
        if hi < out_ref.shape[1]:
            out_ref[rows, hi:] = jnp.zeros((BLOCK, out_ref.shape[1] - hi), jnp.float32)


def first_kernel(shifts, last, row_ref, *refs):
    pieces, (top_out, work_out, sums_out, token_out, work, sums) = refs[:shifts], refs[shifts:]
    height, size = pieces[0].shape
    me = row_ref[0]
    for s in range(shifts):
        source = lax.rem(me - s + shifts, shifts)
        work[pl.ds(pl.multiple_of(source * height, 8), height), :] = pieces[s][...]
    factor_steps(work, sums, top_out, 0, 0, last, size // BLOCK)
    work_out[...] = work[last * BLOCK :, last * BLOCK :]
    sums_out[...] = sums[last * BLOCK :, : last * BLOCK]
    token_out[...] = jnp.zeros_like(token_out)


def second_kernel(first, token_in, work_in, sums_in, bottom_out, work, sums):
    size = bottom_out.shape[1]
    work[...] = work_in[...]
    sums[:, : first * BLOCK] = sums_in[...]
    factor_steps(work, sums, bottom_out, first * BLOCK, first, size // BLOCK, size // BLOCK)


def first_half(row, pieces):
    size = pieces[0].shape[1]
    last = size // BLOCK // 2
    cut = last * BLOCK
    rest = size - cut
    return pl.pallas_call(
        functools.partial(first_kernel, len(pieces), last),
        out_shape=(
            jax.ShapeDtypeStruct((cut, cut), jnp.float32),
            jax.ShapeDtypeStruct((rest, rest), jnp.float32),
            jax.ShapeDtypeStruct((rest, cut), jnp.float32),
            TOKEN,
        ),
        in_specs=[SMEM] + [VMEM] * len(pieces),
        out_specs=(VMEM,) * 4,
        scratch_shapes=[pltpu.VMEM((size, size), jnp.float32)] * 2,
        cost_estimate=pl.CostEstimate(flops=50 * size**3, bytes_accessed=8 * size * size, transcendentals=0),
        compiler_params=memory(4 * size * size),
        name="first_half",
    )(row, *pieces)


def second_half(token, work, sums):
    rest, cut = sums.shape
    size = rest + cut
    return pl.pallas_call(
        functools.partial(second_kernel, cut // BLOCK),
        out_shape=jax.ShapeDtypeStruct((rest, size), jnp.float32),
        in_specs=[VMEM] * 3,
        out_specs=VMEM,
        scratch_shapes=[pltpu.VMEM((rest, rest), jnp.float32), pltpu.VMEM((rest, size), jnp.float32)],
        cost_estimate=pl.CostEstimate(flops=50 * size**3, bytes_accessed=8 * size * size, transcendentals=0),
        compiler_params=memory(4 * size * size),
        name="second_half",
    )(token, work, sums)


def pack_kernel(place_ref, diag_ref, b_ref, a_ref, plane_out, panel_out):
    core = place_ref[1]
    rows = b_ref.shape[0]
    half = plane_out.shape[0] - 2 * rows
    plane_out[:half] = diag_ref[pl.ds(pl.multiple_of(core * half, 8), half), :]
    plane_out[half : half + rows] = b_ref[...]
    plane_out[half + rows :] = a_ref[...]
    panel_out[:rows] = b_ref[...]
    panel_out[rows:] = a_ref[...]


def pack(places, a_diag, b_panel, a_panel, cores):
    rows, size = b_panel.shape
    half = a_diag.shape[0] // cores
    return pl.pallas_call(
        pack_kernel,
        out_shape=(
            jax.ShapeDtypeStruct((half + 2 * rows, size), jnp.float32),
            jax.ShapeDtypeStruct((2 * rows, size), jnp.float32),
        ),
        in_specs=[SMEM] + [VMEM] * 3,
        out_specs=(VMEM,) * 2,
        compiler_params=memory(4 * a_diag.size + 4 * b_panel.size),
        name="pack",
    )(places, a_diag, b_panel, a_panel)


def route_kernel(count, chips, place_ref, *refs):
    planes, panels, refs = refs[:count], refs[count : count + chips], refs[count + chips + 1 :]
    diag_out, rows_out, sends, token_out, held = refs[0], refs[1], refs[2:-2], refs[-2], refs[-1]
    token_out[...] = jnp.zeros_like(token_out)
    row, chip, slot = place_ref[0], place_ref[2], place_ref[3]
    half = diag_out.shape[1]
    for s in range(count):
        source = lax.rem(row - s + count, count)
        diag_out[source] = planes[s][:half]
        held[source] = planes[s][half:]
    for s in range(chips):
        rows_out[lax.rem(chip - s + chips, chips)] = panels[s][...]
    for s in range(chips):
        sends[s][...] = held[lax.rem(slot + s, chips)]


def route(token, places, planes, panels):
    count, chips = len(planes), len(panels)
    both, size = panels[0].shape
    half = planes[0].shape[0] - both
    shape = jax.ShapeDtypeStruct
    outs = [shape((count, half, size), jnp.float32), shape((chips, both, size), jnp.float32)]
    outs += [shape((both, size), jnp.float32)] * chips + [TOKEN]
    found = pl.pallas_call(
        functools.partial(route_kernel, count, chips),
        out_shape=tuple(outs),
        in_specs=[SMEM] + [VMEM] * (count + chips + 1),
        out_specs=(VMEM,) * len(outs),
        scratch_shapes=[pltpu.VMEM((count, both, size), jnp.float32)],
        compiler_params=memory(2 * count * planes[0].size + 3 * chips * both * size),
        name="route",
    )(places, *planes, *panels, token)
    return found[0], found[1], list(found[2:-1]), found[-1]


def split(value):
    high = value.astype(jnp.bfloat16)
    return high, (value - high.astype(jnp.float32)).astype(jnp.bfloat16)


def product(left, right, dims):
    def dot(x, y):
        return lax.dot_general(x, y, (dims, ((), ())), preferred_element_type=jnp.float32)

    return dot(left[0], right[0]) + (dot(left[0], right[1]) + dot(left[1], right[0]))


NT = ((1,), (1,))
NN = ((1,), (0,))


def update_kernel(place_ref, *refs):
    top_ref, bottom_ref, diag_ref, diag_other, rows_ref, rows_other, trail_ref = refs[:7]
    chips = rows_ref.shape[0]
    pieces = refs[7 : 7 + chips]
    diag_out, low_out, panel_out, trail_out, inverse_work, diag_work, rows_work, cols_work = refs[7 + chips :]
    row, core, chip, place = place_ref[0], place_ref[1], place_ref[2], place_ref[4]
    count, half, size = diag_ref.shape
    cores = 2
    rows = rows_ref.shape[1] // 2
    height = cores * half
    cut = top_ref.shape[0]
    for r in range(count):
        diag_work[pl.ds(pl.multiple_of(r * height + core * half, 8), half), :] = diag_ref[r]
        diag_work[pl.ds(pl.multiple_of(r * height + (1 - core) * half, 8), half), :] = diag_other[r]
    for z in range(chips):
        mine = pl.ds(pl.multiple_of((z * cores + core) * rows, 8), rows)
        theirs = pl.ds(pl.multiple_of((z * cores + 1 - core) * rows, 8), rows)
        spot = pl.ds(pl.multiple_of(lax.rem(chip - z + chips, chips) * rows, 8), rows)
        for which in range(2):
            part = slice(which * rows, (which + 1) * rows)
            rows_work[which, mine, :] = rows_ref[z, part]
            rows_work[which, theirs, :] = rows_other[z, part]
            cols_work[which, spot, :] = pieces[z][part]
    inverse_work[:cut, :cut] = top_ref[...]
    inverse_work[:cut, cut:] = jnp.zeros((cut, size - cut), jnp.float32)
    inverse_work[cut:, :] = bottom_ref[...]

    inverse = split(inverse_work[...])
    left = split(product(inverse, split(diag_work[...]), NN))
    reduced = product(left, inverse, NT)
    diag_work[...] = reduced
    diag_out[...] = diag_work[pl.ds(pl.multiple_of(row * height, 8), height), :]
    reduced = split(reduced)

    def panel(work):
        low = product(split(work[0]), inverse, NT)
        correction = 0.5 * product(split(low), reduced, NN)
        mixed = product(split(work[1]), inverse, NT) - correction
        return low, mixed, correction

    low_rows, mixed_rows, correction = panel(rows_work)
    rows_work[0] = low_rows
    rows_work[1] = mixed_rows - correction
    mine = pl.ds(pl.multiple_of(place * rows, 8), rows)
    low_out[...] = rows_work[0, mine, :]
    panel_out[...] = rows_work[1, mine, :]
    low_cols, mixed_cols, _ = panel(cols_work)
    trail_out[...] = trail_ref[...] - (
        product(split(mixed_rows), split(low_cols), NT) + product(split(low_rows), split(mixed_cols), NT)
    )


def update(places, top, bottom, diag, diag_other, own, other, a_trail, pieces, shapes):
    size = bottom.shape[1]
    height, width = a_trail.shape
    return pl.pallas_call(
        update_kernel,
        out_shape=tuple(jax.ShapeDtypeStruct(shape, jnp.float32) for shape in shapes),
        in_specs=[SMEM] + [VMEM] * (7 + len(pieces)),
        out_specs=(VMEM,) * 4,
        scratch_shapes=[
            pltpu.VMEM((size, size), jnp.float32),
            pltpu.VMEM((size, size), jnp.float32),
            pltpu.VMEM((2, height, size), jnp.float32),
            pltpu.VMEM((2, width, size), jnp.float32),
        ],
        cost_estimate=pl.CostEstimate(flops=10 * size**3, bytes_accessed=8 * size * size, transcendentals=0),
        compiler_params=memory(3 * size * size + 4 * height * size + 4 * width * size + 2 * height * width),
        name="update",
    )(places, top, bottom, diag, diag_other, own, other, a_trail, *pieces)


def body(b_diag, a_diag, b_panel, a_panel, a_trail):
    count, chips, cores = (lax.axis_size(name) for name in ("row", "chip", "core"))
    row, chip, core = (lax.axis_index(name) for name in ("row", "chip", "core"))
    rows, _ = b_panel.shape
    height, width = a_trail.shape
    assert chips == count and height == chips * cores * rows and width * cores == height
    span = chips // cores
    slot = lax.rem(chip, span) * cores + core

    def shift(array, axis, s):
        n = lax.axis_size(axis)
        return lax.ppermute(array, axis, [(i, (i + s) % n) for i in range(n)])

    def swap(array):
        return lax.ppermute(array, "core", [(0, 1), (1, 0)])

    places = jnp.stack([row, core, chip, slot, chip * cores + core]).astype(jnp.int32)
    b_pieces = [b_diag] + [shift(b_diag, "row", s) for s in range(1, count)]
    plane, panel = pack(places, a_diag, b_panel, a_panel, cores)
    panels = [panel] + [shift(panel, "chip", s) for s in range(1, chips)]
    planes = [plane] + [shift(plane, "row", s) for s in range(1, count)]
    top, work, sums, token = first_half(places, b_pieces)
    diag, own, sends, token = route(token, places, planes, panels)
    pieces = []
    for s in range(chips):
        pairs = []
        for r in range(count):
            for z in range(chips):
                for c in range(cores):
                    target = ((z % span) * cores + c + s) % chips
                    pairs.append(((r * chips + z) * cores + c, (r * chips + target) * cores + z // span))
        pieces.append(lax.ppermute(sends[s], ("row", "chip", "core"), pairs))
    diag_other, other = swap(diag), swap(own)
    bottom = second_half(token, work, sums)
    shapes = (a_diag.shape, b_panel.shape, a_panel.shape, a_trail.shape)
    return update(places, top, bottom, diag, diag_other, own, other, a_trail, pieces, shapes)


def solution(mesh):
    count, cols = mesh.devices.shape
    cores = 2
    fine = Mesh(mesh.devices.reshape(count, cols // cores, cores), ("row", "chip", "core"))
    in_specs = (
        P("row", None),
        P("row", None),
        P(("row", "chip", "core"), None),
        P(("row", "chip", "core"), None),
        P("row", ("chip", "core")),
    )
    out_specs = (
        P("row", None),
        P(("row", "chip", "core"), None),
        P(("row", "chip", "core"), None),
        P("row", ("chip", "core")),
    )
    return jax.shard_map(body, mesh=fine, in_specs=in_specs, out_specs=out_specs, check_vma=False)
```

```python
import functools

import jax
import jax.numpy as jnp
from jax import lax
from jax.experimental import pallas as pl
from jax.experimental.pallas import tpu as pltpu
from jax.sharding import Mesh
from jax.sharding import PartitionSpec as P


HIGHEST = lax.Precision.HIGHEST
SMALL = 32
BLOCK = 128
TOKEN = jax.ShapeDtypeStruct((8, 128), jnp.float32)
VMEM = pl.BlockSpec(memory_space=pltpu.VMEM)
SMEM = pl.BlockSpec(memory_space=pltpu.SMEM)


def memory(*elements):
    return pltpu.CompilerParams(vmem_limit_bytes=min(2**23 + 12 * sum(elements), 60 * 2**20))


def nt(left, right):
    return lax.dot_general(
        left, right, (((1,), (1,)), ((), ())), precision=HIGHEST, preferred_element_type=jnp.float32
    )


def nn(left, right):
    return lax.dot_general(
        left, right, (((1,), (0,)), ((), ())), precision=HIGHEST, preferred_element_type=jnp.float32
    )


def invert_small(block, offset):
    lanes = block.shape[1]
    groups = SMALL // 8
    cols = []
    for m in range(SMALL):
        column = block[:, offset + m : offset + m + 1]
        cols.append(
            [
                jnp.broadcast_to(column[8 * h : 8 * h + 8], (8, lanes)) if h >= m // 8 else None
                for h in range(groups)
            ]
        )
    sublane = lax.broadcasted_iota(jnp.int32, (8, lanes), 0)
    lane = lax.broadcasted_iota(jnp.int32, (8, lanes), 1)
    rows = [jnp.where(lane == sublane + (offset + 8 * h), 1.0, 0.0).astype(jnp.float32) for h in range(groups)]
    pivots = [None] * groups

    def spread_row(value, s):
        return jnp.broadcast_to(value[s : s + 1, :], (8, lanes))

    for j in range(SMALL):
        g = j // 8
        c = cols[j]
        pivot = spread_row(c[g], j % 8)
        scale = 1.0 / pivot
        pivots[g] = pivot if j % 8 == 0 else jnp.where(sublane == j % 8, pivot, pivots[g])
        row = spread_row(rows[g], j % 8)
        low = [None if c[h] is None else c[h] * scale for h in range(groups)]
        for m in range(j + 1, SMALL):
            t = spread_row(c[m // 8], m % 8)
            for h in range(m // 8, groups):
                if m == j + 1:
                    cols[m][h] = cols[m][h] - (c[h] * t) * scale
                else:
                    cols[m][h] = cols[m][h] - low[h] * t
        for h in range(g, groups):
            factor = jnp.where(sublane > j % 8, low[h], 0.0) if h == g else low[h]
            rows[h] = rows[h] - factor * row
    return jnp.concatenate([rows[h] * lax.rsqrt(pivots[h]) for h in range(groups)], axis=0)


def invert_block(block):
    size = block.shape[0]
    done = []
    total = None
    for b in range(size // SMALL):
        offset = b * SMALL
        below = offset + SMALL
        small = invert_small(block[offset:below, :], offset)
        last = below == size
        if not last:
            low = nt(block[below:, :], small)
            full = jnp.concatenate([jnp.zeros((below, SMALL), jnp.float32), low], axis=0)
            block = jnp.concatenate([block[:below], block[below:, :] - nt(low, full)], axis=0)
        strip = small if total is None else small - nn(small, total)
        done.append(strip)
        if not last:
            update = nn(full, strip)
            total = update if total is None else total + update
    return jnp.concatenate(done, axis=0)


def factor_steps(work, sums, out_ref, base, first, last, count):
    start = first * BLOCK
    for k in range(first, last):
        lo, hi = k * BLOCK, (k + 1) * BLOCK
        here = slice(lo - base, hi - base)
        rows = slice(lo - start, hi - start)
        inverse = invert_block(work[here, here])
        out_ref[rows, lo:hi] = inverse
        if k + 1 < count:
            below = slice(hi - base, count * BLOCK - base)
            low = nt(work[below, here], inverse)
            for i in range(k + 1, count):
                part = slice(i * BLOCK - base, (i + 1) * BLOCK - base)
                wide = slice(hi - base, (i + 1) * BLOCK - base)
                mine = low[i * BLOCK - hi : (i + 1) * BLOCK - hi]
                work[part, wide] = work[part, wide] - nt(mine, low[: (i + 1) * BLOCK - hi])
        if k > 0:
            out_ref[rows, :lo] = -nn(inverse, sums[here, :lo])
        if k + 1 < count:
            update = nn(low, out_ref[rows, :hi])
            if k > 0:
                sums[below, :lo] = sums[below, :lo] + update[:, :lo]
            sums[below, lo:hi] = update[:, lo:hi]
        if hi < out_ref.shape[1]:
            out_ref[rows, hi:] = jnp.zeros((BLOCK, out_ref.shape[1] - hi), jnp.float32)


def gather_square(work, core, me, count, own, ops, swapped, last, last_swapped, holder):
    height = own.shape[0]

    def place(source, piece):
        work[pl.ds(pl.multiple_of(source * height, 8), height), :] = piece[...]

    place(me, own)
    for j in range(len(ops)):
        place(me ^ (2 * j + 1 + core), ops[j])
        place(me ^ (2 * j + 2 - core), swapped[j])

    @pl.when(core == holder)
    def _():
        place(me ^ (count - 1), last)

    @pl.when(core != holder)
    def _():
        place(me ^ (count - 1), last_swapped)


def step_kernel(count, first, last, place_ref, *refs):
    if first == 0:
        own, final, final_swapped = refs[:3]
        extra = count // 2 - 1
        ops, swapped = refs[3 : 3 + extra], refs[3 + extra : 3 + 2 * extra]
        refs = refs[3 + 2 * extra :]
    else:
        _, work_in, sums_in = refs[:3]
        refs = refs[3:]
    inverse_out, work, sums = refs[0], refs[-2], refs[-1]
    total, size = inverse_out.shape[1] // BLOCK, work.shape[0]
    if first == 0:
        gather_square(work, place_ref[1], place_ref[0], count, own, ops, swapped, final, final_swapped, 0)
        total = size // BLOCK
    else:
        work[...] = work_in[...]
        sums[:, : first * BLOCK] = sums_in[...]
        total = first + size // BLOCK
    factor_steps(work, sums, inverse_out, first * BLOCK, first, last, total)
    if last < total:
        work_out, sums_out, token_out = refs[1:4]
        cut = (last - first) * BLOCK
        work_out[...] = work[cut:, cut:]
        sums_out[...] = sums[cut:, : last * BLOCK]
        token_out[...] = jnp.zeros_like(token_out)


def factor_part(places, operands, count, first, last, total):
    shape = jax.ShapeDtypeStruct
    size = (total - first) * BLOCK
    rest = (total - last) * BLOCK
    made = last * BLOCK
    outs = [shape(((last - first) * BLOCK, made), jnp.float32)]
    if rest:
        outs += [shape((rest, rest), jnp.float32), shape((rest, made), jnp.float32), TOKEN]
    return pl.pallas_call(
        functools.partial(step_kernel, count, first, last),
        out_shape=tuple(outs),
        in_specs=[SMEM] + [VMEM] * len(operands),
        out_specs=(VMEM,) * len(outs),
        scratch_shapes=[pltpu.VMEM((size, size), jnp.float32), pltpu.VMEM((size, total * BLOCK), jnp.float32)],
        cost_estimate=pl.CostEstimate(flops=10**10, bytes_accessed=8 * size * size, transcendentals=0),
        compiler_params=memory(4 * size * size),
    )(places, *operands)


def pack_kernel(place_ref, b_diag, a_diag, b_panel, a_panel, last_out, panel_out, sems):
    rows = b_panel.shape[0]
    upper = pltpu.make_async_copy(b_panel, panel_out.at[pl.ds(0, rows)], sems.at[0])
    lower = pltpu.make_async_copy(a_panel, panel_out.at[pl.ds(rows, rows)], sems.at[1])
    upper.start()
    lower.start()

    @pl.when(place_ref[1] == 0)
    def _():
        copy = pltpu.make_async_copy(b_diag, last_out, sems.at[2])
        copy.start()
        copy.wait()

    @pl.when(place_ref[1] != 0)
    def _():
        copy = pltpu.make_async_copy(a_diag, last_out, sems.at[3])
        copy.start()
        copy.wait()

    upper.wait()
    lower.wait()


def pack(places, b_diag, a_diag, b_panel, a_panel):
    rows, size = b_panel.shape
    return pl.pallas_call(
        pack_kernel,
        out_shape=(
            jax.ShapeDtypeStruct(b_diag.shape, jnp.float32),
            jax.ShapeDtypeStruct((2 * rows, size), jnp.float32),
        ),
        in_specs=[SMEM] + [pl.BlockSpec(memory_space=pltpu.HBM)] * 4,
        out_specs=(VMEM,) * 2,
        scratch_shapes=[pltpu.SemaphoreType.DMA((4,))],
        compiler_params=memory(4 * a_diag.size + 4 * b_panel.size),
        name="pack",
    )(places, b_diag, a_diag, b_panel, a_panel)


def join_kernel(place_ref, own, other, out):
    both = own.shape[0]
    core = place_ref[1]
    out[pl.ds(pl.multiple_of(core * both, 8), both), :] = own[...]
    out[pl.ds(pl.multiple_of((1 - core) * both, 8), both), :] = other[...]


def join(places, own, other):
    both, size = own.shape
    return pl.pallas_call(
        join_kernel,
        out_shape=jax.ShapeDtypeStruct((2 * both, size), jnp.float32),
        in_specs=[SMEM] + [VMEM] * 2,
        out_specs=VMEM,
        compiler_params=memory(4 * own.size),
        name="join",
    )(places, own, other)


def route_kernel(count, chips, place_ref, _, own, last, last_swapped, *refs):
    extra = count // 2 - 1
    ops, swapped = refs[:extra], refs[extra : 2 * extra]
    sends, token_out, held = refs[2 * extra : -2], refs[-2], refs[-1]
    row, core, slot = place_ref[0], place_ref[1], place_ref[3]
    token_out[...] = jnp.zeros_like(token_out)
    held[row] = own[...]
    for j in range(extra):
        held[row ^ (2 * j + 1 + core)] = ops[j][...]
        held[row ^ (2 * j + 2 - core)] = swapped[j][...]

    @pl.when(core == 0)
    def _():
        held[row ^ (count - 1)] = last[...]

    @pl.when(core != 0)
    def _():
        held[row ^ (count - 1)] = last_swapped[...]

    for t in range(len(sends)):
        sends[t][...] = held[lax.rem(slot + 2 * t, chips)]


def route(places, token, own, last, last_swapped, ops, swapped, count, chips):
    shape = jax.ShapeDtypeStruct
    outs = [shape(own.shape, jnp.float32)] * (chips // 2) + [TOKEN]
    found = pl.pallas_call(
        functools.partial(route_kernel, count, chips),
        out_shape=tuple(outs),
        in_specs=[SMEM] + [VMEM] * (4 + len(ops) + len(swapped)),
        out_specs=(VMEM,) * len(outs),
        scratch_shapes=[pltpu.VMEM((count,) + own.shape, jnp.float32)],
        compiler_params=memory(2 * (count + chips) * own.size),
        name="route",
    )(places, token, own, last, last_swapped, *ops, *swapped)
    return list(found[:-1]), found[-1]


def split(value):
    high = value.astype(jnp.bfloat16)
    return high, (value - high.astype(jnp.float32)).astype(jnp.bfloat16)


def product(left, right, dims):
    def dot(x, y):
        return lax.dot_general(x, y, (dims, ((), ())), preferred_element_type=jnp.float32)

    return dot(left[0], right[0]) + (dot(left[0], right[1]) + dot(left[1], right[0]))


NT = ((1,), (1,))
NN = ((1,), (0,))


def update_kernel(count, chips, parts, place_ref, *refs):
    inverses, refs = refs[:parts], refs[parts:]
    (diag, square, square_swapped, panel, final, final_swapped, trail_ref), refs = refs[:7], refs[7:]
    extra, more, pairs = count // 2 - 1, chips // 2 - 1, chips // 2
    groups = []
    for n in (extra, extra, more, more, pairs):
        groups.append(refs[:n])
        refs = refs[n:]
    diag_ops, diag_swapped, row_ops, row_swapped, pieces = groups
    diag_out, low_out, panel_out, trail_out, inverse_work, diag_work, rows_work, cols_work = refs
    row, core, chip, place = place_ref[0], place_ref[1], place_ref[2], place_ref[4]
    height, size = diag.shape
    rows = panel.shape[0] // 4
    gather_square(diag_work, core, row, count, diag, diag_ops, diag_swapped, square, square_swapped, 1)

    def store(work, spot, piece):
        for c in range(2):
            for which in range(2):
                part = slice((2 * c + which) * rows, (2 * c + which + 1) * rows)
                work[which, pl.ds(pl.multiple_of((2 * spot + c) * rows, 8), rows), :] = piece[part]

    store(rows_work, chip, panel)
    for j in range(more):
        store(rows_work, chip ^ (2 * j + 1 + core), row_ops[j])
        store(rows_work, chip ^ (2 * j + 2 - core), row_swapped[j])

    @pl.when(core == 1)
    def _():
        store(rows_work, chip ^ (chips - 1), final)

    @pl.when(core != 1)
    def _():
        store(rows_work, chip ^ (chips - 1), final_swapped)

    for t in range(pairs):
        store(cols_work, lax.rem(chip - 2 * t + chips, chips) // 2, pieces[t])
    at = 0
    for part in inverses:
        tall, wide = part.shape
        inverse_work[at : at + tall, :wide] = part[...]
        if wide < size:
            inverse_work[at : at + tall, wide:] = jnp.zeros((tall, size - wide), jnp.float32)
        at += tall

    inverse = split(inverse_work[...])
    left = split(product(inverse, split(diag_work[...]), NN))
    reduced = product(left, inverse, NT)
    diag_work[...] = reduced
    diag_out[...] = diag_work[pl.ds(pl.multiple_of(row * height, 8), height), :]
    reduced = split(reduced)

    def panel(work):
        low = product(split(work[0]), inverse, NT)
        correction = 0.5 * product(split(low), reduced, NN)
        mixed = product(split(work[1]), inverse, NT) - correction
        return low, mixed, correction

    low_rows, mixed_rows, correction = panel(rows_work)
    rows_work[0] = low_rows
    rows_work[1] = mixed_rows - correction
    mine = pl.ds(pl.multiple_of(place * rows, 8), rows)
    low_out[...] = rows_work[0, mine, :]
    panel_out[...] = rows_work[1, mine, :]
    low_cols, mixed_cols, _ = panel(cols_work)
    trail_out[...] = trail_ref[...] - (
        product(split(mixed_rows), split(low_cols), NT) + product(split(low_rows), split(mixed_cols), NT)
    )


def update(places, inverses, singles, groups, count, chips, shapes):
    size = inverses[-1].shape[1]
    height, width = shapes[-1]
    operands = list(inverses) + list(singles) + [piece for group in groups for piece in group]
    return pl.pallas_call(
        functools.partial(update_kernel, count, chips, len(inverses)),
        out_shape=tuple(jax.ShapeDtypeStruct(shape, jnp.float32) for shape in shapes),
        in_specs=[SMEM] + [VMEM] * len(operands),
        out_specs=(VMEM,) * 4,
        scratch_shapes=[
            pltpu.VMEM((size, size), jnp.float32),
            pltpu.VMEM((size, size), jnp.float32),
            pltpu.VMEM((2, height, size), jnp.float32),
            pltpu.VMEM((2, width, size), jnp.float32),
        ],
        cost_estimate=pl.CostEstimate(flops=10**10, bytes_accessed=8 * size * size, transcendentals=0),
        compiler_params=memory(3 * size * size + 4 * height * size + 4 * width * size + 2 * height * width),
        name="update",
    )(places, *operands)


def body(b_diag, a_diag, b_panel, a_panel, a_trail):
    count, chips, cores = (lax.axis_size(name) for name in ("row", "chip", "core"))
    row, chip, core = (lax.axis_index(name) for name in ("row", "chip", "core"))
    rows, size = b_panel.shape
    height, width = a_trail.shape
    assert cores == 2 and chips == count and height == chips * cores * rows and width * cores == height
    assert count & (count - 1) == 0
    span = chips // cores

    def exchange(array, target):
        pairs = []
        for r in range(count):
            for z in range(chips):
                for c in range(cores):
                    to = target(r, z, c)
                    pairs.append(((r * chips + z) * cores + c, (to[0] * chips + to[1]) * cores + to[2]))
        return lax.ppermute(array, ("row", "chip", "core"), pairs)

    def to_rows(array, j):
        return exchange(array, lambda r, z, c: (r ^ (2 * j + 1 + c), z, c))

    def to_chips(array, j):
        return exchange(array, lambda r, z, c: (r, z ^ (2 * j + 1 + c), c))

    def swap(array):
        return exchange(array, lambda r, z, c: (r, z, 1 - c))

    slot = lax.rem(chip, span) * 2 + core
    places = jnp.stack([row, core, chip, slot, chip * 2 + core]).astype(jnp.int32)
    extra, more = range(count // 2 - 1), range(chips // 2 - 1)
    b_ops = [to_rows(b_diag, j) for j in extra]
    mixed, own = pack(places, b_diag, a_diag, b_panel, a_panel)
    other = swap(own)
    square = exchange(mixed, lambda r, z, c: (r ^ (count - 1), z, c))
    panel = join(places, own, other)
    p_ops = [to_rows(panel, j) for j in extra]
    final = exchange(panel, lambda r, z, c: (r, z ^ (chips - 1), c) if c else (r ^ (count - 1), z, c))
    z_ops = [to_chips(panel, j) for j in more]
    a_ops = [to_rows(a_diag, j) for j in extra]
    b_swapped = [swap(x) for x in b_ops]
    square_swapped = swap(square)
    total = size // BLOCK
    cuts = (0, total // 4, total // 2, total)
    top, work, sums, token = factor_part(
        places, [b_diag, square, square_swapped, *b_ops, *b_swapped], count, cuts[0], cuts[1], total
    )
    p_swapped = [swap(x) for x in p_ops]
    final_swapped = swap(final)
    middle, work, sums, token = factor_part(places, [token, work, sums], count, cuts[1], cuts[2], total)
    sends, token = route(places, token, panel, final, final_swapped, p_ops, p_swapped, count, chips)
    pieces = [
        exchange(
            sends[t], lambda r, z, c: (r, ((z % span) * 2 + c + 2 * t) % chips, z // span)
        )
        for t in range(span)
    ]
    z_swapped = [swap(x) for x in z_ops]
    a_swapped = [swap(x) for x in a_ops]
    (bottom,) = factor_part(places, [token, work, sums], count, cuts[2], cuts[3], total)
    shapes = (a_diag.shape, b_panel.shape, a_panel.shape, a_trail.shape)
    singles = (a_diag, square, square_swapped, panel, final, final_swapped, a_trail)
    groups = (a_ops, a_swapped, z_ops, z_swapped, pieces)
    return update(places, (top, middle, bottom), singles, groups, count, chips, shapes)


def solution(mesh):
    count, cols = mesh.devices.shape
    cores = 2
    fine = Mesh(mesh.devices.reshape(count, cols // cores, cores), ("row", "chip", "core"))
    in_specs = (
        P("row", None),
        P("row", None),
        P(("row", "chip", "core"), None),
        P(("row", "chip", "core"), None),
        P("row", ("chip", "core")),
    )
    out_specs = (
        P("row", None),
        P(("row", "chip", "core"), None),
        P(("row", "chip", "core"), None),
        P("row", ("chip", "core")),
    )
    return jax.shard_map(body, mesh=fine, in_specs=in_specs, out_specs=out_specs, check_vma=False)
```

```python
import functools

import jax
import jax.numpy as jnp
from jax import lax
from jax.experimental import pallas as pl
from jax.experimental.pallas import tpu as pltpu
from jax.sharding import Mesh
from jax.sharding import PartitionSpec as P


HIGHEST = lax.Precision.HIGHEST
SMALL = 32
BLOCK = 128
TOKEN = jax.ShapeDtypeStruct((8, 128), jnp.float32)
VMEM = pl.BlockSpec(memory_space=pltpu.VMEM)
SMEM = pl.BlockSpec(memory_space=pltpu.SMEM)


def memory(*elements):
    return pltpu.CompilerParams(vmem_limit_bytes=min(2**23 + 12 * sum(elements), 60 * 2**20))


def nt(left, right):
    return lax.dot_general(
        left, right, (((1,), (1,)), ((), ())), precision=HIGHEST, preferred_element_type=jnp.float32
    )


def nn(left, right):
    return lax.dot_general(
        left, right, (((1,), (0,)), ((), ())), precision=HIGHEST, preferred_element_type=jnp.float32
    )


def invert_small(block, offset):
    lanes = block.shape[1]
    groups = SMALL // 8
    cols = []
    for m in range(SMALL):
        column = block[:, offset + m : offset + m + 1]
        cols.append(
            [
                jnp.broadcast_to(column[8 * h : 8 * h + 8], (8, lanes)) if h >= m // 8 else None
                for h in range(groups)
            ]
        )
    sublane = lax.broadcasted_iota(jnp.int32, (8, lanes), 0)
    lane = lax.broadcasted_iota(jnp.int32, (8, lanes), 1)
    rows = [jnp.where(lane == sublane + (offset + 8 * h), 1.0, 0.0).astype(jnp.float32) for h in range(groups)]
    pivots = [None] * groups

    def spread_row(value, s):
        return jnp.broadcast_to(value[s : s + 1, :], (8, lanes))

    for j in range(SMALL):
        g = j // 8
        c = cols[j]
        pivot = spread_row(c[g], j % 8)
        scale = 1.0 / pivot
        pivots[g] = pivot if j % 8 == 0 else jnp.where(sublane == j % 8, pivot, pivots[g])
        row = spread_row(rows[g], j % 8)
        low = [None if c[h] is None else c[h] * scale for h in range(groups)]
        for m in range(j + 1, SMALL):
            t = spread_row(c[m // 8], m % 8)
            for h in range(m // 8, groups):
                if m == j + 1:
                    cols[m][h] = cols[m][h] - (c[h] * t) * scale
                else:
                    cols[m][h] = cols[m][h] - low[h] * t
        for h in range(g, groups):
            factor = jnp.where(sublane > j % 8, low[h], 0.0) if h == g else low[h]
            rows[h] = rows[h] - factor * row
    return jnp.concatenate([rows[h] * lax.rsqrt(pivots[h]) for h in range(groups)], axis=0)


def invert_block(block):
    size = block.shape[0]
    done = []
    total = None
    for b in range(size // SMALL):
        offset = b * SMALL
        below = offset + SMALL
        small = invert_small(block[offset:below, :], offset)
        last = below == size
        if not last:
            low = nt(block[below:, :], small)
            full = jnp.concatenate([jnp.zeros((below, SMALL), jnp.float32), low], axis=0)
            block = jnp.concatenate([block[:below], block[below:, :] - nt(low, full)], axis=0)
        strip = small if total is None else small - nn(small, total)
        done.append(strip)
        if not last:
            update = nn(full, strip)
            total = update if total is None else total + update
    return jnp.concatenate(done, axis=0)


def factor_steps(work, sums, out_ref, base, first, last, count):
    start = first * BLOCK
    for k in range(first, last):
        lo, hi = k * BLOCK, (k + 1) * BLOCK
        here = slice(lo - base, hi - base)
        rows = slice(lo - start, hi - start)
        inverse = invert_block(work[here, here])
        out_ref[rows, lo:hi] = inverse
        if k + 1 < count:
            below = slice(hi - base, count * BLOCK - base)
            low = nt(work[below, here], inverse)
            for i in range(k + 1, count):
                part = slice(i * BLOCK - base, (i + 1) * BLOCK - base)
                wide = slice(hi - base, (i + 1) * BLOCK - base)
                mine = low[i * BLOCK - hi : (i + 1) * BLOCK - hi]
                work[part, wide] = work[part, wide] - nt(mine, low[: (i + 1) * BLOCK - hi])
        if k > 0:
            out_ref[rows, :lo] = -nn(inverse, sums[here, :lo])
        if k + 1 < count:
            update = nn(low, out_ref[rows, :hi])
            if k > 0:
                sums[below, :lo] = sums[below, :lo] + update[:, :lo]
            sums[below, lo:hi] = update[:, lo:hi]
        if hi < out_ref.shape[1]:
            out_ref[rows, hi:] = jnp.zeros((BLOCK, out_ref.shape[1] - hi), jnp.float32)


def gather_square(work, core, me, count, own, ops, swapped, last, last_swapped):
    height = own.shape[0]

    def place(source, piece):
        work[pl.ds(pl.multiple_of(source * height, 8), height), :] = piece[...]

    place(me, own)
    for j in range(len(ops)):
        place(me ^ (2 * j + 1 + core), ops[j])
        place(me ^ (2 * j + 2 - core), swapped[j])

    if last_swapped is None:
        place(me ^ (count - 1), last)
        return

    @pl.when(core == 0)
    def _():
        place(me ^ (count - 1), last)

    @pl.when(core != 0)
    def _():
        place(me ^ (count - 1), last_swapped)


def step_kernel(count, first, last, place_ref, *refs):
    if first == 0:
        own, final, final_swapped = refs[:3]
        extra = count // 2 - 1
        ops, swapped = refs[3 : 3 + extra], refs[3 + extra : 3 + 2 * extra]
        refs = refs[3 + 2 * extra :]
    else:
        _, work_in, sums_in = refs[:3]
        refs = refs[3:]
    inverse_out, work, sums = refs[0], refs[-2], refs[-1]
    total, size = inverse_out.shape[1] // BLOCK, work.shape[0]
    if first == 0:
        gather_square(work, place_ref[1], place_ref[0], count, own, ops, swapped, final, final_swapped)
        total = size // BLOCK
    else:
        work[...] = work_in[...]
        sums[:, : first * BLOCK] = sums_in[...]
        total = first + size // BLOCK
    factor_steps(work, sums, inverse_out, first * BLOCK, first, last, total)
    if last < total:
        work_out, sums_out, token_out = refs[1:4]
        cut = (last - first) * BLOCK
        work_out[...] = work[cut:, cut:]
        sums_out[...] = sums[cut:, : last * BLOCK]
        token_out[...] = jnp.zeros_like(token_out)


def factor_part(places, operands, count, first, last, total):
    shape = jax.ShapeDtypeStruct
    size = (total - first) * BLOCK
    rest = (total - last) * BLOCK
    made = last * BLOCK
    outs = [shape(((last - first) * BLOCK, made), jnp.float32)]
    if rest:
        outs += [shape((rest, rest), jnp.float32), shape((rest, made), jnp.float32), TOKEN]
    return pl.pallas_call(
        functools.partial(step_kernel, count, first, last),
        out_shape=tuple(outs),
        in_specs=[SMEM] + [VMEM] * len(operands),
        out_specs=(VMEM,) * len(outs),
        scratch_shapes=[pltpu.VMEM((size, size), jnp.float32), pltpu.VMEM((size, total * BLOCK), jnp.float32)],
        cost_estimate=pl.CostEstimate(flops=10**10, bytes_accessed=8 * size * size, transcendentals=0),
        compiler_params=memory(4 * size * size),
    )(places, *operands)


def join_kernel(place_ref, b_own, a_own, b_other, a_other, out):
    rows = b_own.shape[0]
    core = place_ref[1]
    for k, piece in enumerate((b_own, a_own)):
        out[pl.ds(pl.multiple_of((2 * core + k) * rows, 8), rows), :] = piece[...]
    for k, piece in enumerate((b_other, a_other)):
        out[pl.ds(pl.multiple_of((2 - 2 * core + k) * rows, 8), rows), :] = piece[...]


def join(places, *pieces):
    rows, size = pieces[0].shape
    return pl.pallas_call(
        join_kernel,
        out_shape=jax.ShapeDtypeStruct((4 * rows, size), jnp.float32),
        in_specs=[SMEM] + [VMEM] * 4,
        out_specs=VMEM,
        compiler_params=memory(8 * pieces[0].size),
        name="join",
    )(places, *pieces)


def route_kernel(count, chips, place_ref, _, own, last, last_swapped, *refs):
    extra = count // 2 - 1
    ops, swapped = refs[:extra], refs[extra : 2 * extra]
    sends, token_out, held = refs[2 * extra : -2], refs[-2], refs[-1]
    row, core, slot = place_ref[0], place_ref[1], place_ref[3]
    token_out[...] = jnp.zeros_like(token_out)
    held[row] = own[...]
    for j in range(extra):
        held[row ^ (2 * j + 1 + core)] = ops[j][...]
        held[row ^ (2 * j + 2 - core)] = swapped[j][...]

    @pl.when(core == 0)
    def _():
        held[row ^ (count - 1)] = last[...]

    @pl.when(core != 0)
    def _():
        held[row ^ (count - 1)] = last_swapped[...]

    for t in range(len(sends)):
        sends[t][...] = held[lax.rem(slot + 2 * t, chips)]


def route(places, token, own, last, last_swapped, ops, swapped, count, chips):
    shape = jax.ShapeDtypeStruct
    outs = [shape(own.shape, jnp.float32)] * (chips // 2) + [TOKEN]
    found = pl.pallas_call(
        functools.partial(route_kernel, count, chips),
        out_shape=tuple(outs),
        in_specs=[SMEM] + [VMEM] * (4 + len(ops) + len(swapped)),
        out_specs=(VMEM,) * len(outs),
        scratch_shapes=[pltpu.VMEM((count,) + own.shape, jnp.float32)],
        compiler_params=memory(2 * (count + chips) * own.size),
        name="route",
    )(places, token, own, last, last_swapped, *ops, *swapped)
    return list(found[:-1]), found[-1]


def split(value):
    high = value.astype(jnp.bfloat16)
    return high, (value - high.astype(jnp.float32)).astype(jnp.bfloat16)


def product(left, right, dims):
    def dot(x, y):
        return lax.dot_general(x, y, (dims, ((), ())), preferred_element_type=jnp.float32)

    return dot(left[0], right[0]) + (dot(left[0], right[1]) + dot(left[1], right[0]))


NT = ((1,), (1,))
NN = ((1,), (0,))


def update_kernel(count, chips, parts, place_ref, *refs):
    inverses, refs = refs[:parts], refs[parts:]
    (diag, square, panel, final, final_swapped, trail_ref), refs = refs[:6], refs[6:]
    extra, more, pairs = count // 2 - 1, chips // 2 - 1, chips // 2
    groups = []
    for n in (extra, extra, more, more, pairs):
        groups.append(refs[:n])
        refs = refs[n:]
    diag_ops, diag_swapped, row_ops, row_swapped, pieces = groups
    diag_out, low_out, panel_out, trail_out, inverse_work, diag_work, rows_work, cols_work = refs
    row, core, chip, place = place_ref[0], place_ref[1], place_ref[2], place_ref[4]
    height, size = diag.shape
    rows = panel.shape[0] // 4
    gather_square(diag_work, core, row, count, diag, diag_ops, diag_swapped, square, None)

    def store(work, spot, piece):
        for c in range(2):
            for which in range(2):
                part = slice((2 * c + which) * rows, (2 * c + which + 1) * rows)
                work[which, pl.ds(pl.multiple_of((2 * spot + c) * rows, 8), rows), :] = piece[part]

    store(rows_work, chip, panel)
    for j in range(more):
        store(rows_work, chip ^ (2 * j + 1 + core), row_ops[j])
        store(rows_work, chip ^ (2 * j + 2 - core), row_swapped[j])

    @pl.when(core == 1)
    def _():
        store(rows_work, chip ^ (chips - 1), final)

    @pl.when(core != 1)
    def _():
        store(rows_work, chip ^ (chips - 1), final_swapped)

    for t in range(pairs):
        store(cols_work, lax.rem(chip - 2 * t + chips, chips) // 2, pieces[t])
    at = 0
    for part in inverses:
        tall, wide = part.shape
        inverse_work[at : at + tall, :wide] = part[...]
        if wide < size:
            inverse_work[at : at + tall, wide:] = jnp.zeros((tall, size - wide), jnp.float32)
        at += tall

    inverse = split(inverse_work[...])
    left = split(product(inverse, split(diag_work[...]), NN))
    reduced = product(left, inverse, NT)
    diag_work[...] = reduced
    diag_out[...] = diag_work[pl.ds(pl.multiple_of(row * height, 8), height), :]
    reduced = split(reduced)

    def panel(work):
        low = product(split(work[0]), inverse, NT)
        correction = 0.5 * product(split(low), reduced, NN)
        mixed = product(split(work[1]), inverse, NT) - correction
        return low, mixed, correction

    low_rows, mixed_rows, correction = panel(rows_work)
    rows_work[0] = low_rows
    rows_work[1] = mixed_rows - correction
    mine = pl.ds(pl.multiple_of(place * rows, 8), rows)
    low_out[...] = rows_work[0, mine, :]
    panel_out[...] = rows_work[1, mine, :]
    low_cols, mixed_cols, _ = panel(cols_work)
    trail_out[...] = trail_ref[...] - (
        product(split(mixed_rows), split(low_cols), NT) + product(split(low_rows), split(mixed_cols), NT)
    )


def update(places, inverses, singles, groups, count, chips, shapes):
    size = inverses[-1].shape[1]
    height, width = shapes[-1]
    operands = list(inverses) + list(singles) + [piece for group in groups for piece in group]
    return pl.pallas_call(
        functools.partial(update_kernel, count, chips, len(inverses)),
        out_shape=tuple(jax.ShapeDtypeStruct(shape, jnp.float32) for shape in shapes),
        in_specs=[SMEM] + [VMEM] * len(operands),
        out_specs=(VMEM,) * 4,
        scratch_shapes=[
            pltpu.VMEM((size, size), jnp.float32),
            pltpu.VMEM((size, size), jnp.float32),
            pltpu.VMEM((2, height, size), jnp.float32),
            pltpu.VMEM((2, width, size), jnp.float32),
        ],
        cost_estimate=pl.CostEstimate(flops=10**10, bytes_accessed=8 * size * size, transcendentals=0),
        compiler_params=memory(3 * size * size + 4 * height * size + 4 * width * size + 2 * height * width),
        name="update",
    )(places, *operands)


def body(b_diag, a_diag, b_panel, a_panel, a_trail):
    count, chips, cores = (lax.axis_size(name) for name in ("row", "chip", "core"))
    row, chip, core = (lax.axis_index(name) for name in ("row", "chip", "core"))
    rows, size = b_panel.shape
    height, width = a_trail.shape
    assert cores == 2 and chips == count and height == chips * cores * rows and width * cores == height
    assert count & (count - 1) == 0
    span = chips // cores

    def exchange(array, target):
        pairs = []
        for r in range(count):
            for z in range(chips):
                for c in range(cores):
                    to = target(r, z, c)
                    if to is None:
                        continue
                    pairs.append(((r * chips + z) * cores + c, (to[0] * chips + to[1]) * cores + to[2]))
        return lax.ppermute(array, ("row", "chip", "core"), pairs)

    def to_rows(array, j):
        return exchange(array, lambda r, z, c: (r ^ (2 * j + 1 + c), z, c))

    def to_chips(array, j):
        return exchange(array, lambda r, z, c: (r, z ^ (2 * j + 1 + c), c))

    def swap(array):
        return exchange(array, lambda r, z, c: (r, z, 1 - c))

    slot = lax.rem(chip, span) * 2 + core
    places = jnp.stack([row, core, chip, slot, chip * 2 + core]).astype(jnp.int32)
    extra, more = range(count // 2 - 1), range(chips // 2 - 1)
    b_ops = [to_rows(b_diag, j) for j in extra]
    square = exchange(b_diag, lambda r, z, c: None if c else (r ^ (count - 1), z, c))
    b_other, a_other = swap(b_panel), swap(a_panel)
    panel = join(places, b_panel, a_panel, b_other, a_other)
    p_ops = [to_rows(panel, j) for j in extra]
    final = exchange(panel, lambda r, z, c: (r, z ^ (chips - 1), c) if c else (r ^ (count - 1), z, c))
    z_ops = [to_chips(panel, j) for j in more]
    b_swapped = [swap(x) for x in b_ops]
    square_swapped = swap(square)
    a_ops = [to_rows(a_diag, j) for j in extra]
    a_last = exchange(a_diag, lambda r, z, c: (r ^ (count - 1), z, c))
    total = size // BLOCK
    cuts = (0, total // 4, total // 2, total)
    top, work, sums, token = factor_part(
        places, [b_diag, square, square_swapped, *b_ops, *b_swapped], count, cuts[0], cuts[1], total
    )
    p_swapped = [swap(x) for x in p_ops]
    final_swapped = swap(final)
    middle, work, sums, token = factor_part(places, [token, work, sums], count, cuts[1], cuts[2], total)
    sends, token = route(places, token, panel, final, final_swapped, p_ops, p_swapped, count, chips)
    pieces = [
        exchange(
            sends[t], lambda r, z, c: (r, ((z % span) * 2 + c + 2 * t) % chips, z // span)
        )
        for t in range(span)
    ]
    z_swapped = [swap(x) for x in z_ops]
    a_swapped = [swap(x) for x in a_ops]
    (bottom,) = factor_part(places, [token, work, sums], count, cuts[2], cuts[3], total)
    shapes = (a_diag.shape, b_panel.shape, a_panel.shape, a_trail.shape)
    singles = (a_diag, a_last, panel, final, final_swapped, a_trail)
    groups = (a_ops, a_swapped, z_ops, z_swapped, pieces)
    return update(places, (top, middle, bottom), singles, groups, count, chips, shapes)


def solution(mesh):
    count, cols = mesh.devices.shape
    cores = 2
    fine = Mesh(mesh.devices.reshape(count, cols // cores, cores), ("row", "chip", "core"))
    in_specs = (
        P("row", None),
        P("row", None),
        P(("row", "chip", "core"), None),
        P(("row", "chip", "core"), None),
        P("row", ("chip", "core")),
    )
    out_specs = (
        P("row", None),
        P(("row", "chip", "core"), None),
        P(("row", "chip", "core"), None),
        P("row", ("chip", "core")),
    )
    return jax.shard_map(body, mesh=fine, in_specs=in_specs, out_specs=out_specs, check_vma=False)
```

```python
import functools

import jax
import jax.numpy as jnp
from jax import lax
from jax.experimental import pallas as pl
from jax.experimental.pallas import tpu as pltpu
from jax.sharding import Mesh
from jax.sharding import PartitionSpec as P


HIGHEST = lax.Precision.HIGHEST
SMALL = 32
BLOCK = 128
TOKEN = jax.ShapeDtypeStruct((8, 128), jnp.float32)
VMEM = pl.BlockSpec(memory_space=pltpu.VMEM)
SMEM = pl.BlockSpec(memory_space=pltpu.SMEM)


def memory(*elements):
    return pltpu.CompilerParams(vmem_limit_bytes=min(2**23 + 12 * sum(elements), 60 * 2**20))


def nt(left, right):
    return lax.dot_general(
        left, right, (((1,), (1,)), ((), ())), precision=HIGHEST, preferred_element_type=jnp.float32
    )


def nn(left, right):
    return lax.dot_general(
        left, right, (((1,), (0,)), ((), ())), precision=HIGHEST, preferred_element_type=jnp.float32
    )


def invert_small(block, offset, columns):
    lanes = block.shape[1]
    groups = SMALL // 8
    cols = []
    for m in range(SMALL):
        column = block[:, offset + m : offset + m + 1]
        cols.append(
            [
                jnp.broadcast_to(column[8 * h : 8 * h + 8], (8, lanes)) if h >= m // 8 else None
                for h in range(groups)
            ]
        )
    sublane = lax.broadcasted_iota(jnp.int32, (8, lanes), 0)
    lane = lax.broadcasted_iota(jnp.int32, (8, lanes), 1)
    rows = [jnp.where(lane == sublane + (offset + 8 * h), 1.0, 0.0).astype(jnp.float32) for h in range(groups)]
    pivots = [None] * groups

    def spread_row(value, s):
        return jnp.broadcast_to(value[s : s + 1, :], (8, lanes))

    for j in range(SMALL):
        g = j // 8
        c = cols[j]
        for h in range(g, groups):
            columns[j, 8 * h : 8 * h + 8, :] = c[h]

        def entry(m, j=j, c=c):
            near = j > 0 and m <= j + 1
            return spread_row(c[m // 8], m % 8) if near else columns[j, pl.ds(m, 8, stride=0), :]

        pivot = entry(j)
        scale = 1.0 / pivot
        pivots[g] = pivot if j % 8 == 0 else jnp.where(sublane == j % 8, pivot, pivots[g])
        row = spread_row(rows[g], j % 8)
        low = [None if c[h] is None else c[h] * scale for h in range(groups)]
        for m in range(j + 1, SMALL):
            t = entry(m)
            for h in range(m // 8, groups):
                if m == j + 1:
                    cols[m][h] = cols[m][h] - (c[h] * t) * scale
                else:
                    cols[m][h] = cols[m][h] - low[h] * t
        for h in range(g, groups):
            factor = jnp.where(sublane > j % 8, low[h], 0.0) if h == g else low[h]
            rows[h] = rows[h] - factor * row
    return jnp.concatenate([rows[h] * lax.rsqrt(pivots[h]) for h in range(groups)], axis=0)


def invert_block(block, columns):
    size = block.shape[0]
    done = []
    total = None
    for b in range(size // SMALL):
        offset = b * SMALL
        below = offset + SMALL
        small = invert_small(block[offset:below, :], offset, columns)
        last = below == size
        if not last:
            low = nt(block[below:, :], small)
            full = jnp.concatenate([jnp.zeros((below, SMALL), jnp.float32), low], axis=0)
            block = jnp.concatenate([block[:below], block[below:, :] - nt(low, full)], axis=0)
        strip = small if total is None else small - nn(small, total)
        done.append(strip)
        if not last:
            update = nn(full, strip)
            total = update if total is None else total + update
    return jnp.concatenate(done, axis=0)


def factor_steps(work, sums, columns, out_ref, base, first, last, count):
    start = first * BLOCK
    for k in range(first, last):
        lo, hi = k * BLOCK, (k + 1) * BLOCK
        here = slice(lo - base, hi - base)
        rows = slice(lo - start, hi - start)
        inverse = invert_block(work[here, here], columns)
        out_ref[rows, lo:hi] = inverse
        if k + 1 < count:
            below = slice(hi - base, count * BLOCK - base)
            low = nt(work[below, here], inverse)
            for i in range(k + 1, count):
                part = slice(i * BLOCK - base, (i + 1) * BLOCK - base)
                wide = slice(hi - base, (i + 1) * BLOCK - base)
                mine = low[i * BLOCK - hi : (i + 1) * BLOCK - hi]
                work[part, wide] = work[part, wide] - nt(mine, low[: (i + 1) * BLOCK - hi])
        if k > 0:
            out_ref[rows, :lo] = -nn(inverse, sums[here, :lo])
        if k + 1 < count:
            update = nn(low, out_ref[rows, :hi])
            if k > 0:
                sums[below, :lo] = sums[below, :lo] + update[:, :lo]
            sums[below, lo:hi] = update[:, lo:hi]
        if hi < out_ref.shape[1]:
            out_ref[rows, hi:] = jnp.zeros((BLOCK, out_ref.shape[1] - hi), jnp.float32)


def gather_square(work, core, me, count, own, ops, swapped, last, last_swapped):
    height = own.shape[0]

    def place(source, piece):
        work[pl.ds(pl.multiple_of(source * height, 8), height), :] = piece[...]

    place(me, own)
    for j in range(len(ops)):
        place(me ^ (2 * j + 1 + core), ops[j])
        place(me ^ (2 * j + 2 - core), swapped[j])

    if last_swapped is None:
        place(me ^ (count - 1), last)
        return

    @pl.when(core == 0)
    def _():
        place(me ^ (count - 1), last)

    @pl.when(core != 0)
    def _():
        place(me ^ (count - 1), last_swapped)


def step_kernel(count, first, last, place_ref, *refs):
    if first == 0:
        own, final, final_swapped = refs[:3]
        extra = count // 2 - 1
        ops, swapped = refs[3 : 3 + extra], refs[3 + extra : 3 + 2 * extra]
        refs = refs[3 + 2 * extra :]
    else:
        _, work_in, sums_in = refs[:3]
        refs = refs[3:]
    inverse_out, work, sums, columns = refs[0], refs[-3], refs[-2], refs[-1]
    total, size = inverse_out.shape[1] // BLOCK, work.shape[0]
    if first == 0:
        gather_square(work, place_ref[1], place_ref[0], count, own, ops, swapped, final, final_swapped)
        total = size // BLOCK
    else:
        work[...] = work_in[...]
        sums[:, : first * BLOCK] = sums_in[...]
        total = first + size // BLOCK
    factor_steps(work, sums, columns, inverse_out, first * BLOCK, first, last, total)
    if last < total:
        work_out, sums_out, token_out = refs[1:4]
        cut = (last - first) * BLOCK
        work_out[...] = work[cut:, cut:]
        sums_out[...] = sums[cut:, : last * BLOCK]
        token_out[...] = jnp.zeros_like(token_out)


def factor_part(places, operands, count, first, last, total):
    shape = jax.ShapeDtypeStruct
    size = (total - first) * BLOCK
    rest = (total - last) * BLOCK
    made = last * BLOCK
    outs = [shape(((last - first) * BLOCK, made), jnp.float32)]
    if rest:
        outs += [shape((rest, rest), jnp.float32), shape((rest, made), jnp.float32), TOKEN]
    return pl.pallas_call(
        functools.partial(step_kernel, count, first, last),
        out_shape=tuple(outs),
        in_specs=[SMEM] + [VMEM] * len(operands),
        out_specs=(VMEM,) * len(outs),
        scratch_shapes=[
            pltpu.VMEM((size, size), jnp.float32),
            pltpu.VMEM((size, total * BLOCK), jnp.float32),
            pltpu.VMEM((SMALL, SMALL, BLOCK), jnp.float32),
        ],
        cost_estimate=pl.CostEstimate(flops=10**10, bytes_accessed=8 * size * size, transcendentals=0),
        compiler_params=memory(4 * size * size),
    )(places, *operands)


def join_kernel(place_ref, b_own, a_own, b_other, a_other, out):
    rows = b_own.shape[0]
    core = place_ref[1]
    for k, piece in enumerate((b_own, a_own)):
        out[pl.ds(pl.multiple_of((2 * core + k) * rows, 8), rows), :] = piece[...]
    for k, piece in enumerate((b_other, a_other)):
        out[pl.ds(pl.multiple_of((2 - 2 * core + k) * rows, 8), rows), :] = piece[...]


def join(places, *pieces):
    rows, size = pieces[0].shape
    return pl.pallas_call(
        join_kernel,
        out_shape=jax.ShapeDtypeStruct((4 * rows, size), jnp.float32),
        in_specs=[SMEM] + [VMEM] * 4,
        out_specs=VMEM,
        compiler_params=memory(8 * pieces[0].size),
        name="join",
    )(places, *pieces)


def route_kernel(count, chips, place_ref, _, own, last, last_swapped, *refs):
    extra = count // 2 - 1
    ops, swapped = refs[:extra], refs[extra : 2 * extra]
    sends, token_out, held = refs[2 * extra : -2], refs[-2], refs[-1]
    row, core, slot = place_ref[0], place_ref[1], place_ref[3]
    token_out[...] = jnp.zeros_like(token_out)
    held[row] = own[...]
    for j in range(extra):
        held[row ^ (2 * j + 1 + core)] = ops[j][...]
        held[row ^ (2 * j + 2 - core)] = swapped[j][...]

    @pl.when(core == 0)
    def _():
        held[row ^ (count - 1)] = last[...]

    @pl.when(core != 0)
    def _():
        held[row ^ (count - 1)] = last_swapped[...]

    for t in range(len(sends)):
        sends[t][...] = held[lax.rem(slot + 2 * t, chips)]


def route(places, token, own, last, last_swapped, ops, swapped, count, chips):
    shape = jax.ShapeDtypeStruct
    outs = [shape(own.shape, jnp.float32)] * (chips // 2) + [TOKEN]
    found = pl.pallas_call(
        functools.partial(route_kernel, count, chips),
        out_shape=tuple(outs),
        in_specs=[SMEM] + [VMEM] * (4 + len(ops) + len(swapped)),
        out_specs=(VMEM,) * len(outs),
        scratch_shapes=[pltpu.VMEM((count,) + own.shape, jnp.float32)],
        compiler_params=memory(2 * (count + chips) * own.size),
        name="route",
    )(places, token, own, last, last_swapped, *ops, *swapped)
    return list(found[:-1]), found[-1]


def split(value):
    high = value.astype(jnp.bfloat16)
    return high, (value - high.astype(jnp.float32)).astype(jnp.bfloat16)


def product(left, right, dims):
    def dot(x, y):
        return lax.dot_general(x, y, (dims, ((), ())), preferred_element_type=jnp.float32)

    return dot(left[0], right[0]) + (dot(left[0], right[1]) + dot(left[1], right[0]))


NT = ((1,), (1,))
NN = ((1,), (0,))


def update_kernel(count, chips, parts, place_ref, *refs):
    inverses, refs = refs[:parts], refs[parts:]
    (diag, square, panel, final, final_swapped, trail_ref), refs = refs[:6], refs[6:]
    extra, more, pairs = count // 2 - 1, chips // 2 - 1, chips // 2
    groups = []
    for n in (extra, extra, more, more, pairs):
        groups.append(refs[:n])
        refs = refs[n:]
    diag_ops, diag_swapped, row_ops, row_swapped, pieces = groups
    diag_out, low_out, panel_out, trail_out, upper_work, diag_work, rows_work, cols_work = refs
    row, core, chip, place = place_ref[0], place_ref[1], place_ref[2], place_ref[4]
    height, _ = diag.shape
    rows = panel.shape[0] // 4
    gather_square(diag_work, core, row, count, diag, diag_ops, diag_swapped, square, None)

    def store(work, spot, piece):
        for c in range(2):
            for which in range(2):
                part = slice((2 * c + which) * rows, (2 * c + which + 1) * rows)
                work[which, pl.ds(pl.multiple_of((2 * spot + c) * rows, 8), rows), :] = piece[part]

    store(rows_work, chip, panel)
    for j in range(more):
        store(rows_work, chip ^ (2 * j + 1 + core), row_ops[j])
        store(rows_work, chip ^ (2 * j + 2 - core), row_swapped[j])

    @pl.when(core == 1)
    def _():
        store(rows_work, chip ^ (chips - 1), final)

    @pl.when(core != 1)
    def _():
        store(rows_work, chip ^ (chips - 1), final_swapped)

    for t in range(pairs):
        store(cols_work, lax.rem(chip - 2 * t + chips, chips) // 2, pieces[t])
    cut = upper_work.shape[0]
    at = 0
    for part in inverses[:-1]:
        tall, wide = part.shape
        upper_work[at : at + tall, :wide] = part[...]
        if wide < cut:
            upper_work[at : at + tall, wide:] = jnp.zeros((tall, cut - wide), jnp.float32)
        at += tall
    upper, lower = split(upper_work[...]), split(inverses[-1][...])

    def back(value):
        parts = split(value)
        first = product([part[:, :cut] for part in parts], upper, NT)
        return jnp.concatenate([first, product(parts, lower, NT)], axis=1)

    diag = split(diag_work[...])
    left = jnp.concatenate([product(upper, [part[:cut] for part in diag], NN), product(lower, diag, NN)], axis=0)
    diag_work[...] = left
    left = split(left)

    def panel(work):
        low = back(work[0])
        change = product(split(low), left, NN)
        start = work[1]
        work[0] = low
        work[1] = start - change
        return split(low), split(back(start - 0.5 * change))

    low_rows, mixed_rows = panel(rows_work)
    low_cols, mixed_cols = panel(cols_work)
    trail_out[...] = trail_ref[...] - (product(mixed_rows, low_cols, NT) + product(low_rows, mixed_cols, NT))
    diag_out[...] = back(diag_work[pl.ds(pl.multiple_of(row * height, 8), height), :])
    mine = pl.ds(pl.multiple_of(place * rows, 8), rows)
    low_out[...] = rows_work[0, mine, :]
    panel_out[...] = back(rows_work[1, mine, :])


def update(places, inverses, singles, groups, count, chips, shapes):
    size = inverses[-1].shape[1]
    height, width = shapes[-1]
    operands = list(inverses) + list(singles) + [piece for group in groups for piece in group]
    return pl.pallas_call(
        functools.partial(update_kernel, count, chips, len(inverses)),
        out_shape=tuple(jax.ShapeDtypeStruct(shape, jnp.float32) for shape in shapes),
        in_specs=[SMEM] + [VMEM] * len(operands),
        out_specs=(VMEM,) * 4,
        scratch_shapes=[
            pltpu.VMEM((size - inverses[-1].shape[0],) * 2, jnp.float32),
            pltpu.VMEM((size, size), jnp.float32),
            pltpu.VMEM((2, height, size), jnp.float32),
            pltpu.VMEM((2, width, size), jnp.float32),
        ],
        cost_estimate=pl.CostEstimate(flops=10**10, bytes_accessed=8 * size * size, transcendentals=0),
        compiler_params=memory(3 * size * size + 4 * height * size + 4 * width * size + 2 * height * width),
        name="update",
    )(places, *operands)


def body(b_diag, a_diag, b_panel, a_panel, a_trail):
    count, chips, cores = (lax.axis_size(name) for name in ("row", "chip", "core"))
    row, chip, core = (lax.axis_index(name) for name in ("row", "chip", "core"))
    rows, size = b_panel.shape
    height, width = a_trail.shape
    assert cores == 2 and chips == count and height == chips * cores * rows and width * cores == height
    assert count & (count - 1) == 0
    span = chips // cores

    def exchange(array, target):
        pairs = []
        for r in range(count):
            for z in range(chips):
                for c in range(cores):
                    to = target(r, z, c)
                    if to is None:
                        continue
                    pairs.append(((r * chips + z) * cores + c, (to[0] * chips + to[1]) * cores + to[2]))
        return lax.ppermute(array, ("row", "chip", "core"), pairs)

    def to_rows(array, j):
        return exchange(array, lambda r, z, c: (r ^ (2 * j + 1 + c), z, c))

    def to_chips(array, j):
        return exchange(array, lambda r, z, c: (r, z ^ (2 * j + 1 + c), c))

    def swap(array):
        return exchange(array, lambda r, z, c: (r, z, 1 - c))

    slot = lax.rem(chip, span) * 2 + core
    places = jnp.stack([row, core, chip, slot, chip * 2 + core]).astype(jnp.int32)
    extra, more = range(count // 2 - 1), range(chips // 2 - 1)
    b_ops = [to_rows(b_diag, j) for j in extra]
    square = exchange(b_diag, lambda r, z, c: None if c else (r ^ (count - 1), z, c))
    b_other, a_other = swap(b_panel), swap(a_panel)
    panel = join(places, b_panel, a_panel, b_other, a_other)
    p_ops = [to_rows(panel, j) for j in extra]
    final = exchange(panel, lambda r, z, c: (r, z ^ (chips - 1), c) if c else (r ^ (count - 1), z, c))
    z_ops = [to_chips(panel, j) for j in more]
    b_swapped = [swap(x) for x in b_ops]
    square_swapped = swap(square)
    a_ops = [to_rows(a_diag, j) for j in extra]
    a_last = exchange(a_diag, lambda r, z, c: (r ^ (count - 1), z, c))
    total = size // BLOCK
    cuts = (0, total // 4, total // 2, total)
    top, work, sums, token = factor_part(
        places, [b_diag, square, square_swapped, *b_ops, *b_swapped], count, cuts[0], cuts[1], total
    )
    p_swapped = [swap(x) for x in p_ops]
    final_swapped = swap(final)
    middle, work, sums, token = factor_part(places, [token, work, sums], count, cuts[1], cuts[2], total)
    sends, token = route(places, token, panel, final, final_swapped, p_ops, p_swapped, count, chips)
    pieces = [
        exchange(
            sends[t], lambda r, z, c: (r, ((z % span) * 2 + c + 2 * t) % chips, z // span)
        )
        for t in range(span)
    ]
    z_swapped = [swap(x) for x in z_ops]
    a_swapped = [swap(x) for x in a_ops]
    (bottom,) = factor_part(places, [token, work, sums], count, cuts[2], cuts[3], total)
    shapes = (a_diag.shape, b_panel.shape, a_panel.shape, a_trail.shape)
    singles = (a_diag, a_last, panel, final, final_swapped, a_trail)
    groups = (a_ops, a_swapped, z_ops, z_swapped, pieces)
    return update(places, (top, middle, bottom), singles, groups, count, chips, shapes)


def solution(mesh):
    count, cols = mesh.devices.shape
    cores = 2
    fine = Mesh(mesh.devices.reshape(count, cols // cores, cores), ("row", "chip", "core"))
    in_specs = (
        P("row", None),
        P("row", None),
        P(("row", "chip", "core"), None),
        P(("row", "chip", "core"), None),
        P("row", ("chip", "core")),
    )
    out_specs = (
        P("row", None),
        P(("row", "chip", "core"), None),
        P(("row", "chip", "core"), None),
        P("row", ("chip", "core")),
    )
    return jax.shard_map(body, mesh=fine, in_specs=in_specs, out_specs=out_specs, check_vma=False)
```

```python
import functools

import jax
import jax.numpy as jnp
from jax import lax
from jax.experimental import pallas as pl
from jax.experimental.pallas import tpu as pltpu
from jax.sharding import Mesh
from jax.sharding import PartitionSpec as P


HIGHEST = lax.Precision.HIGHEST
SMALL = 32
BLOCK = 128
TOKEN = jax.ShapeDtypeStruct((8, 128), jnp.float32)
VMEM = pl.BlockSpec(memory_space=pltpu.VMEM)
SMEM = pl.BlockSpec(memory_space=pltpu.SMEM)


def memory(*elements):
    return pltpu.CompilerParams(vmem_limit_bytes=min(2**23 + 12 * sum(elements), 60 * 2**20))


def nt(left, right):
    return lax.dot_general(
        left, right, (((1,), (1,)), ((), ())), precision=HIGHEST, preferred_element_type=jnp.float32
    )


def nn(left, right):
    return lax.dot_general(
        left, right, (((1,), (0,)), ((), ())), precision=HIGHEST, preferred_element_type=jnp.float32
    )


def invert_small(block, offset, columns):
    lanes = block.shape[1]
    groups = SMALL // 8
    cols = []
    for m in range(SMALL):
        column = block[:, offset + m : offset + m + 1]
        cols.append(
            [
                jnp.broadcast_to(column[8 * h : 8 * h + 8], (8, lanes)) if h >= m // 8 else None
                for h in range(groups)
            ]
        )
    sublane = lax.broadcasted_iota(jnp.int32, (8, lanes), 0)
    lane = lax.broadcasted_iota(jnp.int32, (8, lanes), 1)
    rows = [jnp.where(lane == sublane + (offset + 8 * h), 1.0, 0.0).astype(jnp.float32) for h in range(groups)]
    pivots = [None] * groups

    def spread_row(value, s):
        return jnp.broadcast_to(value[s : s + 1, :], (8, lanes))

    for j in range(SMALL):
        g = j // 8
        c = cols[j]
        for h in range(g, groups):
            columns[j, 8 * h : 8 * h + 8, :] = c[h]

        def entry(m, j=j, c=c):
            near = j > 0 and m <= j + 1
            return spread_row(c[m // 8], m % 8) if near else columns[j, pl.ds(m, 8, stride=0), :]

        pivot = entry(j)
        scale = 1.0 / pivot
        pivots[g] = pivot if j % 8 == 0 else jnp.where(sublane == j % 8, pivot, pivots[g])
        row = spread_row(rows[g], j % 8)
        low = [None if c[h] is None else c[h] * scale for h in range(groups)]
        for m in range(j + 1, SMALL):
            t = entry(m)
            for h in range(m // 8, groups):
                if m == j + 1:
                    cols[m][h] = cols[m][h] - (c[h] * t) * scale
                else:
                    cols[m][h] = cols[m][h] - low[h] * t
        for h in range(g, groups):
            factor = jnp.where(sublane > j % 8, low[h], 0.0) if h == g else low[h]
            rows[h] = rows[h] - factor * row
    return jnp.concatenate([rows[h] * lax.rsqrt(pivots[h]) for h in range(groups)], axis=0)


def invert_block(block, columns, others=()):
    size = block.shape[0]
    done = []
    total = None
    for b in range(size // SMALL):
        offset = b * SMALL
        below = offset + SMALL
        mine = block[offset:below, :]
        if 0 < b <= len(others):
            nothing = jnp.minimum(jnp.abs(others[b - 1]()), 0.0)
            mine = mine + jnp.concatenate([nothing] * (SMALL // 8), axis=0)
        small = invert_small(mine, offset, columns)
        last = below == size
        if not last:
            low = nt(block[below:, :], small)
            full = jnp.concatenate([jnp.zeros((below, SMALL), jnp.float32), low], axis=0)
            block = jnp.concatenate([block[:below], block[below:, :] - nt(low, full)], axis=0)
        strip = small if total is None else small - nn(small, total)
        done.append(strip)
        if not last:
            update = nn(full, strip)
            total = update if total is None else total + update
    return jnp.concatenate(done, axis=0)


def factor_steps(work, sums, columns, out_ref, base, pending, first, last, total):
    def at(i, j=None):
        return slice(i * BLOCK - base, (i + 1 if j is None else j) * BLOCK - base)

    def finish(k, inverse):
        spot = slice((k - 1) * BLOCK, k * BLOCK)
        lead = -nn(inverse, sums[at(k), : k * BLOCK])
        out_ref[spot, : k * BLOCK] = lead
        out_ref[spot, k * BLOCK : (k + 1) * BLOCK] = inverse
        if k + 1 < total:
            out_ref[spot, (k + 1) * BLOCK :] = jnp.zeros((BLOCK, (total - k - 1) * BLOCK), jnp.float32)
        return jnp.concatenate([lead, inverse], axis=1)

    for k in range(first, last):
        p = k - 1
        block = work[at(k), at(k)]
        others = []
        if k > 0:
            near = nt(work[at(k), at(p)], pending)
            block = block - nt(near, near)
            held = {}

            def lower(p=p, k=k, held=held, near=near, pending=pending):
                held["strip"] = pending if p == 0 else finish(p, pending)
                held["lows"] = [near] + [nt(work[at(i), at(p)], pending) for i in range(k + 1, total)]
                return held["lows"][-1][:8, :] + held["strip"][:8, :BLOCK]

            def trail(k=k, held=held):
                lows = held["lows"]
                tile = jnp.zeros((8, BLOCK), jnp.float32)
                for i in range(k + 1, total):
                    wide = at(k, i + 1)
                    value = work[at(i), wide] - nt(lows[i - k], jnp.concatenate(lows[: i - k + 1], axis=0))
                    work[at(i), wide] = value
                    tile = tile + value[:8, :BLOCK]
                return tile

            def total_up(p=p, k=k, held=held):
                update = nn(jnp.concatenate(held["lows"], axis=0), held["strip"])
                below = at(k, total)
                if p > 0:
                    sums[below, : p * BLOCK] = sums[below, : p * BLOCK] + update[:, : p * BLOCK]
                sums[below, p * BLOCK : k * BLOCK] = update[:, p * BLOCK :]
                return update[:8, :BLOCK]

            others = [lower, trail, total_up]
        pending = invert_block(block, columns, others)
    if last == total:
        finish(last - 1, pending)
    return pending


def gather_square(work, core, me, count, own, ops, swapped, last, last_swapped):
    height = own.shape[0]

    def place(source, piece):
        work[pl.ds(pl.multiple_of(source * height, 8), height), :] = piece[...]

    place(me, own)
    for j in range(len(ops)):
        place(me ^ (2 * j + 1 + core), ops[j])
        place(me ^ (2 * j + 2 - core), swapped[j])

    if last_swapped is None:
        place(me ^ (count - 1), last)
        return

    @pl.when(core == 0)
    def _():
        place(me ^ (count - 1), last)

    @pl.when(core != 0)
    def _():
        place(me ^ (count - 1), last_swapped)


def step_kernel(count, first, last, total, place_ref, *refs):
    work, sums, columns = refs[-3:]
    if first == 0:
        own, final, final_swapped = refs[:3]
        extra = count // 2 - 1
        ops, swapped = refs[3 : 3 + extra], refs[3 + extra : 3 + 2 * extra]
        outs = refs[3 + 2 * extra : -3]
        gather_square(work, place_ref[1], place_ref[0], count, own, ops, swapped, final, final_swapped)
        pending, base = None, 0
    else:
        _, pending_in, work_in = refs[:3]
        outs = refs[3:-3]
        base = (first - 1) * BLOCK
        work[BLOCK:, :] = work_in[...]
        if base:
            sums[:, :base] = outs[0][...]
            outs = outs[1:]
        pending = pending_in[...]
    pending = factor_steps(work, sums, columns, outs[0], base, pending, first, last, total)
    if last < total:
        pending_out, work_out, token_out = outs[:3]
        pending_out[...] = pending
        cut = last * BLOCK - base
        work_out[...] = work[cut:, cut - BLOCK :]
        token_out[...] = jnp.zeros_like(token_out)
        if last > 1:
            outs[3][...] = sums[cut - BLOCK :, : (last - 1) * BLOCK]


def factor_part(places, operands, count, first, last, total):
    shape = jax.ShapeDtypeStruct
    size = (total - max(first - 1, 0)) * BLOCK
    rest = (total - last) * BLOCK
    if rest:
        outs = [shape((BLOCK, BLOCK), jnp.float32), shape((rest, rest + BLOCK), jnp.float32), TOKEN]
        if last > 1:
            outs.append(shape((rest + BLOCK, (last - 1) * BLOCK), jnp.float32))
    else:
        outs = [shape(((total - 1) * BLOCK, total * BLOCK), jnp.float32)]
    return pl.pallas_call(
        functools.partial(step_kernel, count, first, last, total),
        out_shape=tuple(outs),
        in_specs=[SMEM] + [VMEM] * len(operands),
        out_specs=(VMEM,) * len(outs),
        scratch_shapes=[
            pltpu.VMEM((size, size), jnp.float32),
            pltpu.VMEM((size, total * BLOCK), jnp.float32),
            pltpu.VMEM((SMALL, SMALL, BLOCK), jnp.float32),
        ],
        cost_estimate=pl.CostEstimate(flops=10**10, bytes_accessed=8 * size * size, transcendentals=0),
        compiler_params=memory(4 * size * size),
    )(places, *operands)


def join_kernel(place_ref, b_own, a_own, b_other, a_other, out):
    rows = b_own.shape[0]
    core = place_ref[1]
    for k, piece in enumerate((b_own, a_own)):
        out[pl.ds(pl.multiple_of((2 * core + k) * rows, 8), rows), :] = piece[...]
    for k, piece in enumerate((b_other, a_other)):
        out[pl.ds(pl.multiple_of((2 - 2 * core + k) * rows, 8), rows), :] = piece[...]


def join(places, *pieces):
    rows, size = pieces[0].shape
    return pl.pallas_call(
        join_kernel,
        out_shape=jax.ShapeDtypeStruct((4 * rows, size), jnp.float32),
        in_specs=[SMEM] + [VMEM] * 4,
        out_specs=VMEM,
        compiler_params=memory(8 * pieces[0].size),
        name="join",
    )(places, *pieces)


def route_kernel(count, chips, place_ref, _, own, last, last_swapped, *refs):
    extra = count // 2 - 1
    ops, swapped = refs[:extra], refs[extra : 2 * extra]
    sends, token_out, held = refs[2 * extra : -2], refs[-2], refs[-1]
    row, core, slot = place_ref[0], place_ref[1], place_ref[3]
    token_out[...] = jnp.zeros_like(token_out)
    held[row] = own[...]
    for j in range(extra):
        held[row ^ (2 * j + 1 + core)] = ops[j][...]
        held[row ^ (2 * j + 2 - core)] = swapped[j][...]

    @pl.when(core == 0)
    def _():
        held[row ^ (count - 1)] = last[...]

    @pl.when(core != 0)
    def _():
        held[row ^ (count - 1)] = last_swapped[...]

    for t in range(len(sends)):
        sends[t][...] = held[lax.rem(slot + 2 * t, chips)]


def route(places, token, own, last, last_swapped, ops, swapped, count, chips):
    shape = jax.ShapeDtypeStruct
    outs = [shape(own.shape, jnp.float32)] * (chips // 2) + [TOKEN]
    found = pl.pallas_call(
        functools.partial(route_kernel, count, chips),
        out_shape=tuple(outs),
        in_specs=[SMEM] + [VMEM] * (4 + len(ops) + len(swapped)),
        out_specs=(VMEM,) * len(outs),
        scratch_shapes=[pltpu.VMEM((count,) + own.shape, jnp.float32)],
        compiler_params=memory(2 * (count + chips) * own.size),
        name="route",
    )(places, token, own, last, last_swapped, *ops, *swapped)
    return list(found[:-1]), found[-1]


def split(value):
    high = value.astype(jnp.bfloat16)
    return high, (value - high.astype(jnp.float32)).astype(jnp.bfloat16)


def product(left, right, dims):
    def dot(x, y):
        return lax.dot_general(x, y, (dims, ((), ())), preferred_element_type=jnp.float32)

    return dot(left[0], right[0]) + (dot(left[0], right[1]) + dot(left[1], right[0]))


NT = ((1,), (1,))
NN = ((1,), (0,))


def update_kernel(count, chips, parts, place_ref, *refs):
    inverses, refs = refs[:parts], refs[parts:]
    (diag, square, panel, final, final_swapped, trail_ref), refs = refs[:6], refs[6:]
    extra, more, pairs = count // 2 - 1, chips // 2 - 1, chips // 2
    groups = []
    for n in (extra, extra, more, more, pairs):
        groups.append(refs[:n])
        refs = refs[n:]
    diag_ops, diag_swapped, row_ops, row_swapped, pieces = groups
    diag_out, low_out, panel_out, trail_out, upper_work, diag_work, work = refs
    row, core, chip, place = place_ref[0], place_ref[1], place_ref[2], place_ref[4]
    height, _ = diag.shape
    rows = panel.shape[0] // 4
    gather_square(diag_work, core, row, count, diag, diag_ops, diag_swapped, square, None)

    wide = trail_ref.shape[0]

    def store(start, spot, piece):
        for c in range(2):
            for which in range(2):
                part = slice((2 * c + which) * rows, (2 * c + which + 1) * rows)
                work[which, pl.ds(pl.multiple_of(start + (2 * spot + c) * rows, 8), rows), :] = piece[part]

    store(0, chip, panel)
    for j in range(more):
        store(0, chip ^ (2 * j + 1 + core), row_ops[j])
        store(0, chip ^ (2 * j + 2 - core), row_swapped[j])

    @pl.when(core == 1)
    def _():
        store(0, chip ^ (chips - 1), final)

    @pl.when(core != 1)
    def _():
        store(0, chip ^ (chips - 1), final_swapped)

    for t in range(pairs):
        store(wide, lax.rem(chip - 2 * t + chips, chips) // 2, pieces[t])
    cut = upper_work.shape[0]
    start, rest = inverses
    tall = start.shape[0]
    upper_work[:tall, :tall] = start[...]
    upper_work[:tall, tall:] = jnp.zeros((tall, cut - tall), jnp.float32)
    upper_work[tall:, :] = rest[: cut - tall, :cut]
    upper, lower = split(upper_work[...]), split(rest[cut - tall :, :])

    def halves(value, other, dims):
        cutoff = value[0].shape[0] // 32 * 16
        return jnp.concatenate(
            [product([part[:cutoff] for part in value], other, dims), product([part[cutoff:] for part in value], other, dims)], axis=0
        )

    def back(value):
        parts = split(value)
        first = halves([part[:, :cut] for part in parts], upper, NT)
        return jnp.concatenate([first, halves(parts, lower, NT)], axis=1)

    diag = split(diag_work[...])
    left = jnp.concatenate(
        [halves(upper, [part[:cut] for part in diag], NN), halves(lower, diag, NN)], axis=0
    )
    diag_work[...] = left
    low = back(work[0])
    work[0] = low
    low = split(low)
    change = halves(low, split(left), NN)
    start = work[1]
    work[1] = start - change
    mine = pl.ds(pl.multiple_of(place * rows, 8), rows)
    last = back(
        jnp.concatenate(
            [start - 0.5 * change, work[1, mine, :], diag_work[pl.ds(pl.multiple_of(row * height, 8), height), :]], axis=0
        )
    )
    tall = start.shape[0]
    mixed = split(last[:tall])
    trail_out[...] = trail_ref[...] - (
        halves([part[:wide] for part in mixed], [part[wide:] for part in low], NT)
        + halves([part[:wide] for part in low], [part[wide:] for part in mixed], NT)
    )
    low_out[...] = work[0, mine, :]
    panel_out[...] = last[tall : tall + rows]
    diag_out[...] = last[tall + rows :]


def update(places, inverses, singles, groups, count, chips, shapes):
    size = inverses[-1].shape[1]
    height, width = shapes[-1]
    operands = list(inverses) + list(singles) + [piece for group in groups for piece in group]
    return pl.pallas_call(
        functools.partial(update_kernel, count, chips, len(inverses)),
        out_shape=tuple(jax.ShapeDtypeStruct(shape, jnp.float32) for shape in shapes),
        in_specs=[SMEM] + [VMEM] * len(operands),
        out_specs=(VMEM,) * 4,
        scratch_shapes=[
            pltpu.VMEM((size // 2, size // 2), jnp.float32),
            pltpu.VMEM((size, size), jnp.float32),
            pltpu.VMEM((2, height + width, size), jnp.float32),
        ],
        cost_estimate=pl.CostEstimate(flops=10**10, bytes_accessed=8 * size * size, transcendentals=0),
        compiler_params=memory(3 * size * size + 4 * height * size + 4 * width * size + 2 * height * width),
        name="update",
    )(places, *operands)


def body(b_diag, a_diag, b_panel, a_panel, a_trail):
    count, chips, cores = (lax.axis_size(name) for name in ("row", "chip", "core"))
    row, chip, core = (lax.axis_index(name) for name in ("row", "chip", "core"))
    rows, size = b_panel.shape
    height, width = a_trail.shape
    assert cores == 2 and chips == count and height == chips * cores * rows and width * cores == height
    assert count & (count - 1) == 0
    span = chips // cores

    def exchange(array, target):
        pairs = []
        for r in range(count):
            for z in range(chips):
                for c in range(cores):
                    to = target(r, z, c)
                    if to is None:
                        continue
                    pairs.append(((r * chips + z) * cores + c, (to[0] * chips + to[1]) * cores + to[2]))
        return lax.ppermute(array, ("row", "chip", "core"), pairs)

    def to_rows(array, j):
        return exchange(array, lambda r, z, c: (r ^ (2 * j + 1 + c), z, c))

    def to_chips(array, j):
        return exchange(array, lambda r, z, c: (r, z ^ (2 * j + 1 + c), c))

    def swap(array):
        return exchange(array, lambda r, z, c: (r, z, 1 - c))

    slot = lax.rem(chip, span) * 2 + core
    places = jnp.stack([row, core, chip, slot, chip * 2 + core]).astype(jnp.int32)
    extra, more = range(count // 2 - 1), range(chips // 2 - 1)
    b_ops = [to_rows(b_diag, j) for j in extra]
    square = exchange(b_diag, lambda r, z, c: None if c else (r ^ (count - 1), z, c))
    b_other, a_other = swap(b_panel), swap(a_panel)
    panel = join(places, b_panel, a_panel, b_other, a_other)
    p_ops = [to_rows(panel, j) for j in extra]
    final = exchange(panel, lambda r, z, c: (r, z ^ (chips - 1), c) if c else (r ^ (count - 1), z, c))
    z_ops = [to_chips(panel, j) for j in more]
    b_swapped = [swap(x) for x in b_ops]
    square_swapped = swap(square)
    a_ops = [to_rows(a_diag, j) for j in extra]
    a_last = exchange(a_diag, lambda r, z, c: (r ^ (count - 1), z, c))
    total = size // BLOCK
    cuts = (0, 1, 2, total)
    assert total > 2
    top, work, token = factor_part(
        places, [b_diag, square, square_swapped, *b_ops, *b_swapped], count, cuts[0], cuts[1], total
    )
    p_swapped = [swap(x) for x in p_ops]
    final_swapped = swap(final)
    middle, work, token, sums = factor_part(places, [token, top, work], count, cuts[1], cuts[2], total)
    sends, token = route(places, token, panel, final, final_swapped, p_ops, p_swapped, count, chips)
    pieces = [
        exchange(
            sends[t], lambda r, z, c: (r, ((z % span) * 2 + c + 2 * t) % chips, z // span)
        )
        for t in range(span)
    ]
    z_swapped = [swap(x) for x in z_ops]
    a_swapped = [swap(x) for x in a_ops]
    (bottom,) = factor_part(places, [token, middle, work, sums], count, cuts[2], cuts[3], total)
    shapes = (a_diag.shape, b_panel.shape, a_panel.shape, a_trail.shape)
    singles = (a_diag, a_last, panel, final, final_swapped, a_trail)
    groups = (a_ops, a_swapped, z_ops, z_swapped, pieces)
    return update(places, (top, bottom), singles, groups, count, chips, shapes)


def solution(mesh):
    count, cols = mesh.devices.shape
    cores = 2
    fine = Mesh(mesh.devices.reshape(count, cols // cores, cores), ("row", "chip", "core"))
    in_specs = (
        P("row", None),
        P("row", None),
        P(("row", "chip", "core"), None),
        P(("row", "chip", "core"), None),
        P("row", ("chip", "core")),
    )
    out_specs = (
        P("row", None),
        P(("row", "chip", "core"), None),
        P(("row", "chip", "core"), None),
        P("row", ("chip", "core")),
    )
    return jax.shard_map(body, mesh=fine, in_specs=in_specs, out_specs=out_specs, check_vma=False)
```

```python
import functools

import jax
import jax.numpy as jnp
from jax import lax
from jax.experimental import pallas as pl
from jax.experimental.pallas import tpu as pltpu
from jax.sharding import Mesh
from jax.sharding import PartitionSpec as P


HIGHEST = lax.Precision.HIGHEST
SMALL = 32
BLOCK = 128
TOKEN = jax.ShapeDtypeStruct((8, 128), jnp.float32)
VMEM = pl.BlockSpec(memory_space=pltpu.VMEM)
SMEM = pl.BlockSpec(memory_space=pltpu.SMEM)


def memory(*elements):
    return pltpu.CompilerParams(vmem_limit_bytes=min(2**23 + 12 * sum(elements), 60 * 2**20))


def nt(left, right):
    return lax.dot_general(
        left, right, (((1,), (1,)), ((), ())), precision=HIGHEST, preferred_element_type=jnp.float32
    )


def nn(left, right):
    return lax.dot_general(
        left, right, (((1,), (0,)), ((), ())), precision=HIGHEST, preferred_element_type=jnp.float32
    )


def invert_small(block, offset, columns):
    lanes = block.shape[1]
    groups = SMALL // 8
    cols = []
    for m in range(SMALL):
        column = block[:, offset + m : offset + m + 1]
        cols.append(
            [
                jnp.broadcast_to(column[8 * h : 8 * h + 8], (8, lanes)) if h >= m // 8 else None
                for h in range(groups)
            ]
        )
    sublane = lax.broadcasted_iota(jnp.int32, (8, lanes), 0)
    lane = lax.broadcasted_iota(jnp.int32, (8, lanes), 1)
    rows = [jnp.where(lane == sublane + (offset + 8 * h), 1.0, 0.0).astype(jnp.float32) for h in range(groups)]
    pivots = [None] * groups

    def spread_row(value, s):
        return jnp.broadcast_to(value[s : s + 1, :], (8, lanes))

    for j in range(SMALL):
        g = j // 8
        c = cols[j]
        for h in range(g, groups):
            columns[j, 8 * h : 8 * h + 8, :] = c[h]

        def entry(m, j=j, c=c):
            near = j > 0 and m <= j + 1
            return spread_row(c[m // 8], m % 8) if near else columns[j, pl.ds(m, 8, stride=0), :]

        pivot = entry(j)
        scale = 1.0 / pivot
        pivots[g] = pivot if j % 8 == 0 else jnp.where(sublane == j % 8, pivot, pivots[g])
        row = spread_row(rows[g], j % 8)
        low = [None if c[h] is None else c[h] * scale for h in range(groups)]
        for m in range(j + 1, SMALL):
            t = entry(m)
            for h in range(m // 8, groups):
                if m == j + 1:
                    cols[m][h] = cols[m][h] - (c[h] * t) * scale
                else:
                    cols[m][h] = cols[m][h] - low[h] * t
        for h in range(g, groups):
            factor = jnp.where(sublane > j % 8, low[h], 0.0) if h == g else low[h]
            rows[h] = rows[h] - factor * row
    return jnp.concatenate([rows[h] * lax.rsqrt(pivots[h]) for h in range(groups)], axis=0)


def invert_block(block, columns, others=()):
    size = block.shape[0]
    done = []
    total = None
    for b in range(size // SMALL):
        offset = b * SMALL
        below = offset + SMALL
        mine = block[offset:below, :]
        if 0 < b <= len(others):
            nothing = jnp.minimum(jnp.abs(others[b - 1]()), 0.0)
            mine = mine + jnp.concatenate([nothing] * (SMALL // 8), axis=0)
        small = invert_small(mine, offset, columns)
        last = below == size
        if not last:
            low = nt(block[below:, :], small)
            full = jnp.concatenate([jnp.zeros((below, SMALL), jnp.float32), low], axis=0)
            block = jnp.concatenate([block[:below], block[below:, :] - nt(low, full)], axis=0)
        strip = small if total is None else small - nn(small, total)
        done.append(strip)
        if not last:
            update = nn(full, strip)
            total = update if total is None else total + update
    return jnp.concatenate(done, axis=0)


def factor_steps(work, sums, columns, out_ref, base, pending, first, last, total):
    def at(i, j=None):
        return slice(i * BLOCK - base, (i + 1 if j is None else j) * BLOCK - base)

    def finish(k, inverse):
        spot = slice((k - 1) * BLOCK, k * BLOCK)
        lead = -nn(inverse, sums[at(k), : k * BLOCK])
        out_ref[spot, : k * BLOCK] = lead
        out_ref[spot, k * BLOCK : (k + 1) * BLOCK] = inverse
        if k + 1 < total:
            out_ref[spot, (k + 1) * BLOCK :] = jnp.zeros((BLOCK, (total - k - 1) * BLOCK), jnp.float32)
        return jnp.concatenate([lead, inverse], axis=1)

    for k in range(first, last):
        p = k - 1
        block = work[at(k), at(k)]
        others = []
        if k > 0:
            near = nt(work[at(k), at(p)], pending)
            block = block - nt(near, near)
            held = {}

            def lower(p=p, k=k, held=held, near=near, pending=pending):
                held["strip"] = pending if p == 0 else finish(p, pending)
                held["lows"] = [near] + [nt(work[at(i), at(p)], pending) for i in range(k + 1, total)]
                return held["lows"][-1][:8, :] + held["strip"][:8, :BLOCK]

            def trail(k=k, held=held):
                lows = held["lows"]
                tile = jnp.zeros((8, BLOCK), jnp.float32)
                for i in range(k + 1, total):
                    wide = at(k, i + 1)
                    value = work[at(i), wide] - nt(lows[i - k], jnp.concatenate(lows[: i - k + 1], axis=0))
                    work[at(i), wide] = value
                    tile = tile + value[:8, :BLOCK]
                return tile

            def total_up(p=p, k=k, held=held):
                update = nn(jnp.concatenate(held["lows"], axis=0), held["strip"])
                below = at(k, total)
                if p > 0:
                    sums[below, : p * BLOCK] = sums[below, : p * BLOCK] + update[:, : p * BLOCK]
                sums[below, p * BLOCK : k * BLOCK] = update[:, p * BLOCK :]
                return update[:8, :BLOCK]

            others = [lower, trail, total_up]
        pending = invert_block(block, columns, others)
    if last == total:
        finish(last - 1, pending)
    return pending


def gather_square(work, core, me, count, own, ops, swapped, last, last_swapped):
    height = own.shape[0]

    def place(source, piece):
        work[pl.ds(pl.multiple_of(source * height, 8), height), :] = piece[...]

    place(me, own)
    for j in range(len(ops)):
        place(me ^ (2 * j + 1 + core), ops[j])
        place(me ^ (2 * j + 2 - core), swapped[j])

    if last_swapped is None:
        place(me ^ (count - 1), last)
        return

    @pl.when(core == 0)
    def _():
        place(me ^ (count - 1), last)

    @pl.when(core != 0)
    def _():
        place(me ^ (count - 1), last_swapped)


def step_kernel(count, first, last, total, place_ref, *refs):
    work, sums, columns = refs[-3:]
    if first == 0:
        own, final, final_swapped = refs[:3]
        extra = count // 2 - 1
        ops, swapped = refs[3 : 3 + extra], refs[3 + extra : 3 + 2 * extra]
        outs = refs[3 + 2 * extra : -3]
        gather_square(work, place_ref[1], place_ref[0], count, own, ops, swapped, final, final_swapped)
        pending, base = None, 0
    else:
        _, pending_in, work_in = refs[:3]
        outs = refs[3:-3]
        base = (first - 1) * BLOCK
        work[BLOCK:, :] = work_in[...]
        if base:
            sums[:, :base] = outs[0][...]
            outs = outs[1:]
        pending = pending_in[...]
    pending = factor_steps(work, sums, columns, outs[0], base, pending, first, last, total)
    if last < total:
        pending_out, work_out, token_out = outs[:3]
        pending_out[...] = pending
        cut = last * BLOCK - base
        work_out[...] = work[cut:, cut - BLOCK :]
        token_out[...] = jnp.zeros_like(token_out)
        if last > 1:
            outs[3][...] = sums[cut - BLOCK :, : (last - 1) * BLOCK]


def factor_part(places, operands, count, first, last, total):
    shape = jax.ShapeDtypeStruct
    size = (total - max(first - 1, 0)) * BLOCK
    rest = (total - last) * BLOCK
    if rest:
        outs = [shape((BLOCK, BLOCK), jnp.float32), shape((rest, rest + BLOCK), jnp.float32), TOKEN]
        if last > 1:
            outs.append(shape((rest + BLOCK, (last - 1) * BLOCK), jnp.float32))
    else:
        outs = [shape(((total - 1) * BLOCK, total * BLOCK), jnp.float32)]
    return pl.pallas_call(
        functools.partial(step_kernel, count, first, last, total),
        out_shape=tuple(outs),
        in_specs=[SMEM] + [VMEM] * len(operands),
        out_specs=(VMEM,) * len(outs),
        scratch_shapes=[
            pltpu.VMEM((size, size), jnp.float32),
            pltpu.VMEM((size, total * BLOCK), jnp.float32),
            pltpu.VMEM((SMALL, SMALL, BLOCK), jnp.float32),
        ],
        cost_estimate=pl.CostEstimate(flops=10**10, bytes_accessed=8 * size * size, transcendentals=0),
        compiler_params=memory(4 * size * size),
    )(places, *operands)


def join_kernel(place_ref, own, other, out):
    both = own.shape[0]
    core = place_ref[1]
    out[pl.ds(pl.multiple_of(core * both, 8), both), :] = own[...]
    out[pl.ds(pl.multiple_of((1 - core) * both, 8), both), :] = other[...]


def join(places, own, other):
    both, size = own.shape
    return pl.pallas_call(
        join_kernel,
        out_shape=jax.ShapeDtypeStruct((2 * both, size), jnp.float32),
        in_specs=[SMEM] + [VMEM] * 2,
        out_specs=VMEM,
        compiler_params=memory(4 * own.size),
        name="join",
    )(places, own, other)


def route_kernel(count, chips, place_ref, _, own, last, last_swapped, *refs):
    extra = count // 2 - 1
    ops, swapped = refs[:extra], refs[extra : 2 * extra]
    sends, token_out, held = refs[2 * extra : -2], refs[-2], refs[-1]
    row, core, slot = place_ref[0], place_ref[1], place_ref[3]
    token_out[...] = jnp.zeros_like(token_out)
    held[row] = own[...]
    for j in range(extra):
        held[row ^ (2 * j + 1 + core)] = ops[j][...]
        held[row ^ (2 * j + 2 - core)] = swapped[j][...]

    @pl.when(core == 0)
    def _():
        held[row ^ (count - 1)] = last[...]

    @pl.when(core != 0)
    def _():
        held[row ^ (count - 1)] = last_swapped[...]

    for t in range(len(sends)):
        sends[t][...] = held[lax.rem(slot + 2 * t, chips)]


def route(places, token, own, last, last_swapped, ops, swapped, count, chips):
    shape = jax.ShapeDtypeStruct
    outs = [shape(own.shape, jnp.float32)] * (chips // 2) + [TOKEN]
    found = pl.pallas_call(
        functools.partial(route_kernel, count, chips),
        out_shape=tuple(outs),
        in_specs=[SMEM] + [VMEM] * (4 + len(ops) + len(swapped)),
        out_specs=(VMEM,) * len(outs),
        scratch_shapes=[pltpu.VMEM((count,) + own.shape, jnp.float32)],
        compiler_params=memory(2 * (count + chips) * own.size),
        name="route",
    )(places, token, own, last, last_swapped, *ops, *swapped)
    return list(found[:-1]), found[-1]


def split(value):
    high = value.astype(jnp.bfloat16)
    return high, (value - high.astype(jnp.float32)).astype(jnp.bfloat16)


def product(left, right, dims):
    def dot(x, y):
        return lax.dot_general(x, y, (dims, ((), ())), preferred_element_type=jnp.float32)

    return dot(left[0], right[0]) + (dot(left[0], right[1]) + dot(left[1], right[0]))


NT = ((1,), (1,))
NN = ((1,), (0,))


def update_kernel(count, chips, parts, place_ref, *refs):
    inverses, refs = refs[:parts], refs[parts:]
    (diag, square, panel, final, final_swapped, trail_ref), refs = refs[:6], refs[6:]
    extra, more, pairs = count // 2 - 1, chips // 2 - 1, chips // 2
    groups = []
    for n in (extra, extra, more, more, pairs):
        groups.append(refs[:n])
        refs = refs[n:]
    diag_ops, diag_swapped, row_ops, row_swapped, pieces = groups
    diag_out, low_out, panel_out, trail_out, upper_work, diag_work, work = refs
    row, core, chip, place = place_ref[0], place_ref[1], place_ref[2], place_ref[4]
    height, _ = diag.shape
    rows = panel.shape[0] // 4
    gather_square(diag_work, core, row, count, diag, diag_ops, diag_swapped, square, None)

    wide = trail_ref.shape[0]

    def store(start, spot, piece):
        for c in range(2):
            for which in range(2):
                part = slice((2 * c + which) * rows, (2 * c + which + 1) * rows)
                work[which, pl.ds(pl.multiple_of(start + (2 * spot + c) * rows, 8), rows), :] = piece[part]

    store(0, chip, panel)
    for j in range(more):
        store(0, chip ^ (2 * j + 1 + core), row_ops[j])
        store(0, chip ^ (2 * j + 2 - core), row_swapped[j])

    @pl.when(core == 1)
    def _():
        store(0, chip ^ (chips - 1), final)

    @pl.when(core != 1)
    def _():
        store(0, chip ^ (chips - 1), final_swapped)

    for t in range(pairs):
        store(wide, lax.rem(chip - 2 * t + chips, chips) // 2, pieces[t])
    cut = upper_work.shape[0]
    start, rest = inverses
    tall = start.shape[0]
    upper_work[:tall, :tall] = start[...]
    upper_work[:tall, tall:] = jnp.zeros((tall, cut - tall), jnp.float32)
    upper_work[tall:, :] = rest[: cut - tall, :cut]
    upper, lower = split(upper_work[...]), split(rest[cut - tall :, :])

    def halves(value, other, dims):
        cutoff = value[0].shape[0] // 32 * 16
        return jnp.concatenate(
            [product([part[:cutoff] for part in value], other, dims), product([part[cutoff:] for part in value], other, dims)], axis=0
        )

    def back(value):
        parts = split(value)
        first = halves([part[:, :cut] for part in parts], upper, NT)
        return jnp.concatenate([first, halves(parts, lower, NT)], axis=1)

    diag = split(diag_work[...])
    left = jnp.concatenate(
        [halves(upper, [part[:cut] for part in diag], NN), halves(lower, diag, NN)], axis=0
    )
    diag_work[...] = left
    low = back(work[0])
    work[0] = low
    low = split(low)
    change = halves(low, split(left), NN)
    start = work[1]
    work[1] = start - change
    mine = pl.ds(pl.multiple_of(place * rows, 8), rows)
    last = back(
        jnp.concatenate(
            [start - 0.5 * change, work[1, mine, :], diag_work[pl.ds(pl.multiple_of(row * height, 8), height), :]], axis=0
        )
    )
    tall = start.shape[0]
    mixed = split(last[:tall])
    trail_out[...] = trail_ref[...] - (
        halves([part[:wide] for part in mixed], [part[wide:] for part in low], NT)
        + halves([part[:wide] for part in low], [part[wide:] for part in mixed], NT)
    )
    low_out[...] = work[0, mine, :]
    panel_out[...] = last[tall : tall + rows]
    diag_out[...] = last[tall + rows :]


def update(places, inverses, singles, groups, count, chips, shapes):
    size = inverses[-1].shape[1]
    height, width = shapes[-1]
    operands = list(inverses) + list(singles) + [piece for group in groups for piece in group]
    return pl.pallas_call(
        functools.partial(update_kernel, count, chips, len(inverses)),
        out_shape=tuple(jax.ShapeDtypeStruct(shape, jnp.float32) for shape in shapes),
        in_specs=[SMEM] + [VMEM] * len(operands),
        out_specs=(VMEM,) * 4,
        scratch_shapes=[
            pltpu.VMEM((size // 2, size // 2), jnp.float32),
            pltpu.VMEM((size, size), jnp.float32),
            pltpu.VMEM((2, height + width, size), jnp.float32),
        ],
        cost_estimate=pl.CostEstimate(flops=10**10, bytes_accessed=8 * size * size, transcendentals=0),
        compiler_params=memory(3 * size * size + 4 * height * size + 4 * width * size + 2 * height * width),
        name="update",
    )(places, *operands)


def body(b_diag, a_diag, b_panel, a_panel, a_trail):
    count, chips, cores = (lax.axis_size(name) for name in ("row", "chip", "core"))
    row, chip, core = (lax.axis_index(name) for name in ("row", "chip", "core"))
    rows, size = b_panel.shape
    height, width = a_trail.shape
    assert cores == 2 and chips == count and height == chips * cores * rows and width * cores == height
    assert count & (count - 1) == 0
    span = chips // cores

    def exchange(array, target):
        pairs = []
        for r in range(count):
            for z in range(chips):
                for c in range(cores):
                    to = target(r, z, c)
                    if to is None:
                        continue
                    pairs.append(((r * chips + z) * cores + c, (to[0] * chips + to[1]) * cores + to[2]))
        return lax.ppermute(array, ("row", "chip", "core"), pairs)

    def to_rows(array, j):
        return exchange(array, lambda r, z, c: (r ^ (2 * j + 1 + c), z, c))

    def to_chips(array, j):
        return exchange(array, lambda r, z, c: (r, z ^ (2 * j + 1 + c), c))

    def swap(array):
        return exchange(array, lambda r, z, c: (r, z, 1 - c))

    slot = lax.rem(chip, span) * 2 + core
    places = jnp.stack([row, core, chip, slot, chip * 2 + core]).astype(jnp.int32)
    extra, more = range(count // 2 - 1), range(chips // 2 - 1)
    b_ops = [to_rows(b_diag, j) for j in extra]
    square = exchange(b_diag, lambda r, z, c: None if c else (r ^ (count - 1), z, c))
    own = jnp.concatenate([b_panel, a_panel], axis=0)
    other = swap(own)
    panel = join(places, own, other)
    p_ops = [to_rows(panel, j) for j in extra]
    final = exchange(panel, lambda r, z, c: (r, z ^ (chips - 1), c) if c else (r ^ (count - 1), z, c))
    z_ops = [to_chips(panel, j) for j in more]
    b_swapped = [swap(x) for x in b_ops]
    square_swapped = swap(square)
    a_ops = [to_rows(a_diag, j) for j in extra]
    a_last = exchange(a_diag, lambda r, z, c: (r ^ (count - 1), z, c))
    total = size // BLOCK
    cuts = (0, 1, 2, total)
    assert total > 2
    top, work, token = factor_part(
        places, [b_diag, square, square_swapped, *b_ops, *b_swapped], count, cuts[0], cuts[1], total
    )
    p_swapped = [swap(x) for x in p_ops]
    final_swapped = swap(final)
    middle, work, token, sums = factor_part(places, [token, top, work], count, cuts[1], cuts[2], total)
    sends, token = route(places, token, panel, final, final_swapped, p_ops, p_swapped, count, chips)
    pieces = [
        exchange(
            sends[t], lambda r, z, c: (r, ((z % span) * 2 + c + 2 * t) % chips, z // span)
        )
        for t in range(span)
    ]
    z_swapped = [swap(x) for x in z_ops]
    a_swapped = [swap(x) for x in a_ops]
    (bottom,) = factor_part(places, [token, middle, work, sums], count, cuts[2], cuts[3], total)
    shapes = (a_diag.shape, b_panel.shape, a_panel.shape, a_trail.shape)
    singles = (a_diag, a_last, panel, final, final_swapped, a_trail)
    groups = (a_ops, a_swapped, z_ops, z_swapped, pieces)
    return update(places, (top, bottom), singles, groups, count, chips, shapes)


def solution(mesh):
    count, cols = mesh.devices.shape
    cores = 2
    fine = Mesh(mesh.devices.reshape(count, cols // cores, cores), ("row", "chip", "core"))
    in_specs = (
        P("row", None),
        P("row", None),
        P(("row", "chip", "core"), None),
        P(("row", "chip", "core"), None),
        P("row", ("chip", "core")),
    )
    out_specs = (
        P("row", None),
        P(("row", "chip", "core"), None),
        P(("row", "chip", "core"), None),
        P("row", ("chip", "core")),
    )
    return jax.shard_map(body, mesh=fine, in_specs=in_specs, out_specs=out_specs, check_vma=False)
```

```python
import functools

import jax
import jax.numpy as jnp
from jax import lax
from jax.experimental import pallas as pl
from jax.experimental.pallas import tpu as pltpu
from jax.sharding import Mesh
from jax.sharding import PartitionSpec as P


HIGHEST = lax.Precision.HIGHEST
SMALL = 32
BLOCK = 128
TOKEN = jax.ShapeDtypeStruct((8, 128), jnp.float32)
VMEM = pl.BlockSpec(memory_space=pltpu.VMEM)
SMEM = pl.BlockSpec(memory_space=pltpu.SMEM)


def memory(*elements):
    return pltpu.CompilerParams(vmem_limit_bytes=min(2**23 + 12 * sum(elements), 60 * 2**20))


def nt(left, right):
    return lax.dot_general(
        left, right, (((1,), (1,)), ((), ())), precision=HIGHEST, preferred_element_type=jnp.float32
    )


def nn(left, right):
    return lax.dot_general(
        left, right, (((1,), (0,)), ((), ())), precision=HIGHEST, preferred_element_type=jnp.float32
    )


def invert_small(block, offset, columns):
    lanes = block.shape[1]
    groups = SMALL // 8
    cols = []
    for m in range(SMALL):
        column = block[:, offset + m : offset + m + 1]
        cols.append(
            [
                jnp.broadcast_to(column[8 * h : 8 * h + 8], (8, lanes)) if h >= m // 8 else None
                for h in range(groups)
            ]
        )
    sublane = lax.broadcasted_iota(jnp.int32, (8, lanes), 0)
    lane = lax.broadcasted_iota(jnp.int32, (8, lanes), 1)
    rows = [jnp.where(lane == sublane + (offset + 8 * h), 1.0, 0.0).astype(jnp.float32) for h in range(groups)]
    pivots = [None] * groups

    def spread_row(value, s):
        return jnp.broadcast_to(value[s : s + 1, :], (8, lanes))

    for j in range(SMALL):
        g = j // 8
        c = cols[j]
        for h in range(g, groups):
            columns[j, 8 * h : 8 * h + 8, :] = c[h]

        def entry(m, j=j, c=c):
            near = j > 0 and m <= j + 1
            return spread_row(c[m // 8], m % 8) if near else columns[j, pl.ds(m, 8, stride=0), :]

        pivot = entry(j)
        scale = 1.0 / pivot
        pivots[g] = pivot if j % 8 == 0 else jnp.where(sublane == j % 8, pivot, pivots[g])
        row = spread_row(rows[g], j % 8)
        low = [None if c[h] is None else c[h] * scale for h in range(groups)]
        for m in range(j + 1, SMALL):
            t = entry(m)
            for h in range(m // 8, groups):
                if m == j + 1:
                    cols[m][h] = cols[m][h] - (c[h] * t) * scale
                else:
                    cols[m][h] = cols[m][h] - low[h] * t
        for h in range(g, groups):
            factor = jnp.where(sublane > j % 8, low[h], 0.0) if h == g else low[h]
            rows[h] = rows[h] - factor * row
    return jnp.concatenate([rows[h] * lax.rsqrt(pivots[h]) for h in range(groups)], axis=0)


def invert_block(block, columns, others=(), following=None):
    square = None
    size = block.shape[0]
    done = []
    total = None
    for b in range(size // SMALL):
        offset = b * SMALL
        below = offset + SMALL
        mine = block[offset:below, :]
        if 0 < b <= len(others):
            nothing = jnp.minimum(jnp.abs(others[b - 1]()), 0.0)
            mine = mine + jnp.concatenate([nothing] * (SMALL // 8), axis=0)
        last = below == size
        ahead = None
        if last and following is not None:
            ahead, square = following()
            near = nt(ahead, jnp.concatenate(done, axis=0))
            square = square - nt(near, near)
            ahead = ahead - nt(ahead, total)
        small = invert_small(mine, offset, columns)
        if ahead is not None:
            near = nt(ahead, small)
            square = square - nt(near, near)
        if not last:
            low = nt(block[below:, :], small)
            full = jnp.concatenate([jnp.zeros((below, SMALL), jnp.float32), low], axis=0)
            block = jnp.concatenate([block[:below], block[below:, :] - nt(low, full)], axis=0)
        strip = small if total is None else small - nn(small, total)
        done.append(strip)
        if not last:
            update = nn(full, strip)
            total = update if total is None else total + update
    return jnp.concatenate(done, axis=0), square


def factor_steps(work, sums, columns, out_ref, base, pending, first, last, total):
    def at(i, j=None):
        return slice(i * BLOCK - base, (i + 1 if j is None else j) * BLOCK - base)

    def finish(k, inverse):
        spot = slice((k - 1) * BLOCK, k * BLOCK)
        lead = -nn(inverse, sums[at(k), : k * BLOCK])
        out_ref[spot, : k * BLOCK] = lead
        out_ref[spot, k * BLOCK : (k + 1) * BLOCK] = inverse
        if k + 1 < total:
            out_ref[spot, (k + 1) * BLOCK :] = jnp.zeros((BLOCK, (total - k - 1) * BLOCK), jnp.float32)
        return jnp.concatenate([lead, inverse], axis=1)

    for k in range(first, last):
        p = k - 1
        block = work[at(k), at(k)]
        others = []
        if k > 0:
            near = nt(work[at(k), at(p)], pending)
            if k == first:
                block = block - nt(near, near)
            held = {}

            def lower(p=p, k=k, held=held, near=near, pending=pending):
                held["strip"] = pending if p == 0 else finish(p, pending)
                held["lows"] = [near] + [nt(work[at(i), at(p)], pending) for i in range(k + 1, total)]
                return held["lows"][-1][:8, :] + held["strip"][:8, :BLOCK]

            def trail(k=k, held=held):
                lows = held["lows"]
                tile = jnp.zeros((8, BLOCK), jnp.float32)
                for i in range(k + 1, total):
                    wide = at(k, i + 1)
                    value = work[at(i), wide] - nt(lows[i - k], jnp.concatenate(lows[: i - k + 1], axis=0))
                    work[at(i), wide] = value
                    tile = tile + value[:8, :BLOCK]
                return tile

            def total_up(p=p, k=k, held=held):
                update = nn(jnp.concatenate(held["lows"], axis=0), held["strip"])
                below = at(k, total)
                if p > 0:
                    sums[below, : p * BLOCK] = sums[below, : p * BLOCK] + update[:, : p * BLOCK]
                sums[below, p * BLOCK : k * BLOCK] = update[:, p * BLOCK :]
                return update[:8, :BLOCK]

            others = [lower, trail, total_up]
        following = None
        if k + 1 < last:

            def following(k=k):
                return work[at(k + 1), at(k)], work[at(k + 1), at(k + 1)]

        pending, square = invert_block(block, columns, others, following)
        if k + 1 < last:
            work[at(k + 1), at(k + 1)] = square
    if last == total:
        finish(last - 1, pending)
    return pending


def gather_square(work, core, me, count, own, ops, swapped, last, last_swapped):
    height = own.shape[0]

    def place(source, piece):
        work[pl.ds(pl.multiple_of(source * height, 8), height), :] = piece[...]

    place(me, own)
    for j in range(len(ops)):
        place(me ^ (2 * j + 1 + core), ops[j])
        place(me ^ (2 * j + 2 - core), swapped[j])

    if last_swapped is None:
        place(me ^ (count - 1), last)
        return

    @pl.when(core == 0)
    def _():
        place(me ^ (count - 1), last)

    @pl.when(core != 0)
    def _():
        place(me ^ (count - 1), last_swapped)


def step_kernel(count, first, last, total, place_ref, *refs):
    work, sums, columns = refs[-3:]
    if first == 0:
        own, final, final_swapped = refs[:3]
        extra = count // 2 - 1
        ops, swapped = refs[3 : 3 + extra], refs[3 + extra : 3 + 2 * extra]
        outs = refs[3 + 2 * extra : -3]
        gather_square(work, place_ref[1], place_ref[0], count, own, ops, swapped, final, final_swapped)
        pending, base = None, 0
    else:
        _, pending_in, work_in = refs[:3]
        outs = refs[3:-3]
        base = (first - 1) * BLOCK
        work[BLOCK:, :] = work_in[...]
        if base:
            sums[:, :base] = outs[0][...]
            outs = outs[1:]
        pending = pending_in[...]
    pending = factor_steps(work, sums, columns, outs[0], base, pending, first, last, total)
    if last < total:
        pending_out, work_out, token_out = outs[:3]
        pending_out[...] = pending
        cut = last * BLOCK - base
        work_out[...] = work[cut:, cut - BLOCK :]
        token_out[...] = jnp.zeros_like(token_out)
        if last > 1:
            outs[3][...] = sums[cut - BLOCK :, : (last - 1) * BLOCK]


def factor_part(places, operands, count, first, last, total):
    shape = jax.ShapeDtypeStruct
    size = (total - max(first - 1, 0)) * BLOCK
    rest = (total - last) * BLOCK
    if rest:
        outs = [shape((BLOCK, BLOCK), jnp.float32), shape((rest, rest + BLOCK), jnp.float32), TOKEN]
        if last > 1:
            outs.append(shape((rest + BLOCK, (last - 1) * BLOCK), jnp.float32))
    else:
        outs = [shape(((total - 1) * BLOCK, total * BLOCK), jnp.float32)]
    return pl.pallas_call(
        functools.partial(step_kernel, count, first, last, total),
        out_shape=tuple(outs),
        in_specs=[SMEM] + [VMEM] * len(operands),
        out_specs=(VMEM,) * len(outs),
        scratch_shapes=[
            pltpu.VMEM((size, size), jnp.float32),
            pltpu.VMEM((size, total * BLOCK), jnp.float32),
            pltpu.VMEM((SMALL, SMALL, BLOCK), jnp.float32),
        ],
        cost_estimate=pl.CostEstimate(flops=10**10, bytes_accessed=8 * size * size, transcendentals=0),
        compiler_params=memory(4 * size * size),
    )(places, *operands)


def join_kernel(place_ref, own, other, out):
    both = own.shape[0]
    core = place_ref[1]
    out[pl.ds(pl.multiple_of(core * both, 8), both), :] = own[...]
    out[pl.ds(pl.multiple_of((1 - core) * both, 8), both), :] = other[...]


def join(places, own, other):
    both, size = own.shape
    return pl.pallas_call(
        join_kernel,
        out_shape=jax.ShapeDtypeStruct((2 * both, size), jnp.float32),
        in_specs=[SMEM] + [VMEM] * 2,
        out_specs=VMEM,
        compiler_params=memory(4 * own.size),
        name="join",
    )(places, own, other)


def route_kernel(count, chips, place_ref, _, own, last, last_swapped, *refs):
    extra = count // 2 - 1
    ops, swapped = refs[:extra], refs[extra : 2 * extra]
    sends, token_out, held = refs[2 * extra : -2], refs[-2], refs[-1]
    row, core, slot = place_ref[0], place_ref[1], place_ref[3]
    token_out[...] = jnp.zeros_like(token_out)
    held[row] = own[...]
    for j in range(extra):
        held[row ^ (2 * j + 1 + core)] = ops[j][...]
        held[row ^ (2 * j + 2 - core)] = swapped[j][...]

    @pl.when(core == 0)
    def _():
        held[row ^ (count - 1)] = last[...]

    @pl.when(core != 0)
    def _():
        held[row ^ (count - 1)] = last_swapped[...]

    for t in range(len(sends)):
        sends[t][...] = held[lax.rem(slot + 2 * t, chips)]


def route(places, token, own, last, last_swapped, ops, swapped, count, chips):
    shape = jax.ShapeDtypeStruct
    outs = [shape(own.shape, jnp.float32)] * (chips // 2) + [TOKEN]
    found = pl.pallas_call(
        functools.partial(route_kernel, count, chips),
        out_shape=tuple(outs),
        in_specs=[SMEM] + [VMEM] * (4 + len(ops) + len(swapped)),
        out_specs=(VMEM,) * len(outs),
        scratch_shapes=[pltpu.VMEM((count,) + own.shape, jnp.float32)],
        compiler_params=memory(2 * (count + chips) * own.size),
        name="route",
    )(places, token, own, last, last_swapped, *ops, *swapped)
    return list(found[:-1]), found[-1]


def split(value):
    high = value.astype(jnp.bfloat16)
    return high, (value - high.astype(jnp.float32)).astype(jnp.bfloat16)


def product(left, right, dims):
    def dot(x, y):
        return lax.dot_general(x, y, (dims, ((), ())), preferred_element_type=jnp.float32)

    return dot(left[0], right[0]) + (dot(left[0], right[1]) + dot(left[1], right[0]))


NT = ((1,), (1,))
NN = ((1,), (0,))


def update_kernel(count, chips, parts, place_ref, *refs):
    inverses, refs = refs[:parts], refs[parts:]
    (diag, square, panel, final, final_swapped, trail_ref), refs = refs[:6], refs[6:]
    extra, more, pairs = count // 2 - 1, chips // 2 - 1, chips // 2
    groups = []
    for n in (extra, extra, more, more, pairs):
        groups.append(refs[:n])
        refs = refs[n:]
    diag_ops, diag_swapped, row_ops, row_swapped, pieces = groups
    diag_out, low_out, panel_out, trail_out, upper_work, diag_work, work = refs
    row, core, chip, place = place_ref[0], place_ref[1], place_ref[2], place_ref[4]
    height, _ = diag.shape
    rows = panel.shape[0] // 4
    gather_square(diag_work, core, row, count, diag, diag_ops, diag_swapped, square, None)

    wide = trail_ref.shape[0]

    def store(start, spot, piece):
        for c in range(2):
            for which in range(2):
                part = slice((2 * c + which) * rows, (2 * c + which + 1) * rows)
                work[which, pl.ds(pl.multiple_of(start + (2 * spot + c) * rows, 8), rows), :] = piece[part]

    store(0, chip, panel)
    for j in range(more):
        store(0, chip ^ (2 * j + 1 + core), row_ops[j])
        store(0, chip ^ (2 * j + 2 - core), row_swapped[j])

    @pl.when(core == 1)
    def _():
        store(0, chip ^ (chips - 1), final)

    @pl.when(core != 1)
    def _():
        store(0, chip ^ (chips - 1), final_swapped)

    for t in range(pairs):
        store(wide, lax.rem(chip - 2 * t + chips, chips) // 2, pieces[t])
    cut = upper_work.shape[0]
    start, rest = inverses
    tall = start.shape[0]
    upper_work[:tall, :tall] = start[...]
    upper_work[:tall, tall:] = jnp.zeros((tall, cut - tall), jnp.float32)
    upper_work[tall:, :] = rest[: cut - tall, :cut]
    upper, lower = split(upper_work[...]), split(rest[cut - tall :, :])

    def halves(value, other, dims):
        cutoff = value[0].shape[0] // 32 * 16
        return jnp.concatenate(
            [product([part[:cutoff] for part in value], other, dims), product([part[cutoff:] for part in value], other, dims)], axis=0
        )

    def back(value):
        parts = split(value)
        first = halves([part[:, :cut] for part in parts], upper, NT)
        return jnp.concatenate([first, halves(parts, lower, NT)], axis=1)

    diag = split(diag_work[...])
    left = jnp.concatenate(
        [halves(upper, [part[:cut] for part in diag], NN), halves(lower, diag, NN)], axis=0
    )
    diag_work[...] = left
    low = back(work[0])
    work[0] = low
    low = split(low)
    change = halves(low, split(left), NN)
    start = work[1]
    work[1] = start - change
    mine = pl.ds(pl.multiple_of(place * rows, 8), rows)
    last = back(
        jnp.concatenate(
            [start - 0.5 * change, work[1, mine, :], diag_work[pl.ds(pl.multiple_of(row * height, 8), height), :]], axis=0
        )
    )
    tall = start.shape[0]
    mixed = split(last[:tall])
    trail_out[...] = trail_ref[...] - (
        halves([part[:wide] for part in mixed], [part[wide:] for part in low], NT)
        + halves([part[:wide] for part in low], [part[wide:] for part in mixed], NT)
    )
    low_out[...] = work[0, mine, :]
    panel_out[...] = last[tall : tall + rows]
    diag_out[...] = last[tall + rows :]


def update(places, inverses, singles, groups, count, chips, shapes):
    size = inverses[-1].shape[1]
    height, width = shapes[-1]
    operands = list(inverses) + list(singles) + [piece for group in groups for piece in group]
    return pl.pallas_call(
        functools.partial(update_kernel, count, chips, len(inverses)),
        out_shape=tuple(jax.ShapeDtypeStruct(shape, jnp.float32) for shape in shapes),
        in_specs=[SMEM] + [VMEM] * len(operands),
        out_specs=(VMEM,) * 4,
        scratch_shapes=[
            pltpu.VMEM((size // 2, size // 2), jnp.float32),
            pltpu.VMEM((size, size), jnp.float32),
            pltpu.VMEM((2, height + width, size), jnp.float32),
        ],
        cost_estimate=pl.CostEstimate(flops=10**10, bytes_accessed=8 * size * size, transcendentals=0),
        compiler_params=memory(3 * size * size + 4 * height * size + 4 * width * size + 2 * height * width),
        name="update",
    )(places, *operands)


def body(b_diag, a_diag, b_panel, a_panel, a_trail):
    count, chips, cores = (lax.axis_size(name) for name in ("row", "chip", "core"))
    row, chip, core = (lax.axis_index(name) for name in ("row", "chip", "core"))
    rows, size = b_panel.shape
    height, width = a_trail.shape
    assert cores == 2 and chips == count and height == chips * cores * rows and width * cores == height
    assert count & (count - 1) == 0
    span = chips // cores

    def exchange(array, target):
        pairs = []
        for r in range(count):
            for z in range(chips):
                for c in range(cores):
                    to = target(r, z, c)
                    if to is None:
                        continue
                    pairs.append(((r * chips + z) * cores + c, (to[0] * chips + to[1]) * cores + to[2]))
        return lax.ppermute(array, ("row", "chip", "core"), pairs)

    def to_rows(array, j):
        return exchange(array, lambda r, z, c: (r ^ (2 * j + 1 + c), z, c))

    def to_chips(array, j):
        return exchange(array, lambda r, z, c: (r, z ^ (2 * j + 1 + c), c))

    def swap(array):
        return exchange(array, lambda r, z, c: (r, z, 1 - c))

    slot = lax.rem(chip, span) * 2 + core
    places = jnp.stack([row, core, chip, slot, chip * 2 + core]).astype(jnp.int32)
    extra, more = range(count // 2 - 1), range(chips // 2 - 1)
    b_ops = [to_rows(b_diag, j) for j in extra]
    square = exchange(b_diag, lambda r, z, c: None if c else (r ^ (count - 1), z, c))
    own = jnp.concatenate([b_panel, a_panel], axis=0)
    other = swap(own)
    panel = join(places, own, other)
    p_ops = [to_rows(panel, j) for j in extra]
    final = exchange(panel, lambda r, z, c: (r, z ^ (chips - 1), c) if c else (r ^ (count - 1), z, c))
    z_ops = [to_chips(panel, j) for j in more]
    b_swapped = [swap(x) for x in b_ops]
    square_swapped = swap(square)
    a_ops = [to_rows(a_diag, j) for j in extra]
    a_last = exchange(a_diag, lambda r, z, c: (r ^ (count - 1), z, c))
    total = size // BLOCK
    cuts = (0, 1, 2, total)
    assert total > 2
    top, work, token = factor_part(
        places, [b_diag, square, square_swapped, *b_ops, *b_swapped], count, cuts[0], cuts[1], total
    )
    p_swapped = [swap(x) for x in p_ops]
    final_swapped = swap(final)
    middle, work, token, sums = factor_part(places, [token, top, work], count, cuts[1], cuts[2], total)
    sends, token = route(places, token, panel, final, final_swapped, p_ops, p_swapped, count, chips)
    pieces = [
        exchange(
            sends[t], lambda r, z, c: (r, ((z % span) * 2 + c + 2 * t) % chips, z // span)
        )
        for t in range(span)
    ]
    z_swapped = [swap(x) for x in z_ops]
    a_swapped = [swap(x) for x in a_ops]
    (bottom,) = factor_part(places, [token, middle, work, sums], count, cuts[2], cuts[3], total)
    shapes = (a_diag.shape, b_panel.shape, a_panel.shape, a_trail.shape)
    singles = (a_diag, a_last, panel, final, final_swapped, a_trail)
    groups = (a_ops, a_swapped, z_ops, z_swapped, pieces)
    return update(places, (top, bottom), singles, groups, count, chips, shapes)


def solution(mesh):
    count, cols = mesh.devices.shape
    cores = 2
    fine = Mesh(mesh.devices.reshape(count, cols // cores, cores), ("row", "chip", "core"))
    in_specs = (
        P("row", None),
        P("row", None),
        P(("row", "chip", "core"), None),
        P(("row", "chip", "core"), None),
        P("row", ("chip", "core")),
    )
    out_specs = (
        P("row", None),
        P(("row", "chip", "core"), None),
        P(("row", "chip", "core"), None),
        P("row", ("chip", "core")),
    )
    return jax.shard_map(body, mesh=fine, in_specs=in_specs, out_specs=out_specs, check_vma=False)
```
